32 devices in a mesh: rows: 16 (over z, y, x), tp: 2 (over core).
Axes of the slice: x: 2, y: 2, z: 4, core: 2. Of those that a mesh axis runs over, the one named last changes fastest.
Arguments:
- block_input: float32 [512, 16, 768], P('tp', 'rows'), may hold values from -6 to 6
- cotangent: float32 [512, 16, 768], P('tp', 'rows'), may hold values from -6 to 6
- qkv_weight: float32 [2, 768, 3, 768], P(None, 'rows', None, 'tp'), may hold values from -0.21875 to 0.21875
- proj_weight: float32 [2, 768, 768], P(None, 'tp', 'rows'), may hold values from -0.875 to 0.875
- fc1_weight: float32 [2, 768, 3072], P(None, 'rows', 'tp'), may hold values from -0.21875 to 0.21875
- fc2_weight: float32 [2, 3072, 768], P(None, 'tp', 'rows'), may hold values from -0.109375 to 0.109375
- norm_gains: float32 [2, 2, 768], P(None, None, ('rows', 'tp')), may hold values from 0.5 to 1.5
- biases: float32 [2, 6, 768], P(None, None, ('rows', 'tp')), may hold values from -1.75 to 1.75
- fc1_bias: float32 [2, 3072], P(None, ('rows', 'tp')), may hold values from -1.75 to 1.75
- segments: int32 [16, 512], P('rows'), may hold values from 0 to 7, never falling along the last dimension, each value on 1 to 198 neighbouring positions
- keep_flags: int32 [2, 2, 16, 8], P(None, None, 'rows'), may hold values 0 or 1
Outputs:
- block_output: float32 [512, 16, 768], P('tp', 'rows')
- input_grad: float32 [512, 16, 768], P('tp', 'rows')
- query_key_value_gradient: float32 [2, 768, 3, 768], P(None, 'rows', None, 'tp')
- proj_grad: float32 [2, 768, 768], P(None, 'tp', 'rows')
- expand_weight_gradient: float32 [2, 768, 3072], P(None, 'rows', 'tp')
- fc2_grad: float32 [2, 3072, 768], P(None, 'tp', 'rows')
- gains_grad: float32 [2, 2, 768], P(None, None, ('rows', 'tp'))
- biases_grad: float32 [2, 6, 768], P(None, None, ('rows', 'tp'))
- fc1_bias_grad: float32 [2, 3072], P(None, ('rows', 'tp'))
The draws below stay inside these ranges and needn't reach their ends.
Inputs may be any that keep to these rules, and one draw needn't show every extreme that they name: `segments`: along each packed row the image numbers never decrease; each of the 8 images of a row has 1 to 198 positions, and some image has exactly 198.
All inputs are finite; a program needn't handle non-finite values. No bound on the sum of `keep_flags` on one device may be relied on, other than what follows from the above.
Results may differ from the reference program's by a relative error of at most 0.035.
Values may be sent and summed in bfloat16 or wider, within the bound.
A program may use at most 192 MiB of HBM per device.

```python
import math
import jax
import jax.numpy as jnp
import numpy as np
from jax import lax

D = 768
HEADS = 12
HEAD_DIM = 64
FF = 3072
LAYERS = 2
ROW_LEN = 512
MOST_LEN = 198
SEGS = 8
NROWS = 16


def place_ends(array, key, low, largest):
    shape = array.shape
    spot = [jax.random.randint(jax.random.fold_in(key, axis), (), 0, shape[axis]) for axis in range(len(shape))]
    array = array.at[tuple(spot)].set(low)
    longest = shape.index(max(shape))
    spot[longest] = (spot[longest] + 1) % shape[longest]
    return array.at[tuple(spot)].set(largest)


def block_scale(own_key, shape, shards, least, high):
    def one(position, blocks):
        draws = jax.random.uniform(jax.random.fold_in(jax.random.fold_in(own_key, 6), position), (blocks,), jnp.float32, least / len(shards), high / len(shards))
        return jnp.repeat(jnp.exp(draws), shape[position] // blocks).reshape((-1,) + (1,) * (len(shape) - position - 1))

    gain = one(*shards[0])
    for cut in shards[1:]:
        gain = gain * one(*cut)
    return gain


def split_up(amount, total, limit, skew):
    weights = [(1 << 20) // math.isqrt(rank ** skew) + 1 for rank in range(2, amount + 1)]
    rest, counts = total - limit - (amount - 1), [1] * (amount - 1)
    while rest > 0:
        free = [i for i in range(amount - 1) if counts[i] < limit]
        pool, budget = sum([weights[i] for i in free]), rest
        for i in free:
            addition = min(limit - counts[i], max(1, budget * weights[i] // pool), rest)
            counts[i] = counts[i] + addition
            rest = rest - addition
    return np.array([limit] + counts)


def ragged_sizes(stream_key, number_of, total, reach, lean):
    if number_of == 2:
        one = jax.random.randint(stream_key, (), max(1, total - reach), min(reach, total - 1) + 1)
        return jnp.stack([one, total - one])
    sizes = jnp.asarray(split_up(number_of, total, reach, lean), jnp.int32)
    couples = (number_of - 1) // 2
    donor, receiver = sizes[1:1 + 2 * couples:2], sizes[2:2 + 2 * couples:2]
    room = jnp.minimum(donor - 1, reach - receiver)
    passed = jax.random.randint(jax.random.fold_in(stream_key, 1), (couples,), 0, 1 << 20) % (room + 1)
    sizes = sizes.at[1:1 + 2 * couples:2].set(donor - passed).at[2:2 + 2 * couples:2].set(receiver + passed)
    return sizes[jax.random.permutation(jax.random.fold_in(stream_key, 2), number_of)]


def gaussian(rng, shape, scale, limit, cuts=(), held_as=jnp.bfloat16):
    level = block_scale(rng, shape, cuts, -0.22, 0.18) if cuts else 1.0
    array = jax.random.normal(rng, shape, jnp.float32) * scale * level
    return jnp.minimum(jnp.maximum(array, -limit), limit).astype(held_as)


def setup_inputs(seed: int = 0) -> dict:
    key_list = jax.random.split(jax.random.key(seed), 12)
    block_input = gaussian(key_list[0], (ROW_LEN, NROWS, D), 1.0, 6.0, ((0, 2), (1, 16)), jnp.float32)
    cotangent = gaussian(key_list[1], (ROW_LEN, NROWS, D), 1.0, 6.0, ((0, 2), (1, 16)), jnp.float32)
    qkv_weight = gaussian(key_list[2], (LAYERS, D, 3, D), D ** -0.5, 0.21875, ((1, 16), (3, 2)), jnp.float32)
    proj_weight = gaussian(key_list[3], (LAYERS, D, D), (D // 16) ** -0.5, 0.875, ((1, 2), (2, 16)), jnp.float32)
    fc1_weight = gaussian(key_list[4], (LAYERS, D, FF), D ** -0.5, 0.21875, ((1, 16), (2, 2)), jnp.float32)
    fc2_weight = gaussian(key_list[5], (LAYERS, FF, D), FF ** -0.5, 0.109375, ((1, 2), (2, 16)), jnp.float32)
    norm_gains = jnp.clip(1.0 + 0.1 * jax.random.normal(key_list[6], (LAYERS, 2, D), jnp.float32), 0.5, 1.5)
    biases = gaussian(key_list[7], (LAYERS, 6, D), 0.3, 1.75, ((2, 32),), jnp.float32)
    fc1_bias = gaussian(key_list[8], (LAYERS, FF), 0.3, 1.75, ((1, 32),), jnp.float32)
    segments = jax.vmap(lambda own: jnp.searchsorted(jnp.cumsum(ragged_sizes(own, SEGS, ROW_LEN, MOST_LEN, 1)), jnp.arange(ROW_LEN), side="right"))(jax.random.split(key_list[9], NROWS)).reshape((NROWS, ROW_LEN)).astype(jnp.int32)
    keep_flags = place_ends((jax.random.randint(key_list[10], (LAYERS, 2, NROWS, SEGS), 0, 10) < 9).astype(jnp.int32), jax.random.fold_in(key_list[10], 1), 0, 1)
    return {"block_input": block_input, "cotangent": cotangent, "qkv_weight": qkv_weight, "proj_weight": proj_weight, "fc1_weight": fc1_weight, "fc2_weight": fc2_weight, "norm_gains": norm_gains, "biases": biases, "fc1_bias": fc1_bias, "segments": segments, "keep_flags": keep_flags}


NORM_EPS = 1e-06
KEEP_RATE = 0.9
SCORE_SCALE = 0.125
MASK_FILL = -1e+30
PRECISE = lax.Precision.HIGHEST

@jax.custom_vjp
def low(v):
    return lax.optimization_barrier(v.astype(jnp.bfloat16)).astype(jnp.float32)

@jax.custom_vjp
def reduced_backward(v):
    return v

def low_keep(v):
    return (low(v), None)

def low_pass(kept, grad):
    return (grad,)

def back_keep(v):
    return (v, None)

def back_low(kept, grad):
    return (low(grad),)
low.defvjp(low_keep, low_pass)
reduced_backward.defvjp(back_keep, back_low)

def layer_norm(residual_rows, norm_gain, norm_shift):
    center = residual_rows - lax.optimization_barrier(jnp.mean(residual_rows, axis=-1, keepdims=True))
    spread = lax.optimization_barrier(jnp.mean(center * center, axis=-1, keepdims=True))
    return center * lax.rsqrt(spread + NORM_EPS) * norm_gain + norm_shift

def gain_product(form, left, right):
    return jnp.einsum(form, left, right, precision=PRECISE)

def run_group(residual_rows, seg_group, flag_group, params):
    qkv_w, proj_w, expand_weight, contract_weight, gain_row_block, bias_row_block, expand_bias = params
    length, group_rows, width = residual_rows.shape
    same_image = seg_group[:, :, None] == seg_group[:, None, :]
    member = (seg_group[:, :, None] == jnp.arange(SEGS, dtype=jnp.int32)[None, None, :]).astype(jnp.float32)
    for layer_position in range(LAYERS):
        keep_attn = jnp.transpose(lax.optimization_barrier(jnp.sum(member * flag_group[layer_position, 0][:, None, :], axis=2)))[:, :, None]
        keep_mlp = jnp.transpose(lax.optimization_barrier(jnp.sum(member * flag_group[layer_position, 1][:, None, :], axis=2)))[:, :, None]
        first_normed_rows = low(layer_norm(residual_rows, gain_row_block[layer_position, 0], bias_row_block[layer_position, 0]))
        in_bias = jnp.concatenate([bias_row_block[layer_position, 1], jnp.zeros((width,), jnp.float32), bias_row_block[layer_position, 2]])
        joined = gain_product('trd,dc->trc', first_normed_rows, qkv_w[layer_position].reshape(width, 3 * width)) + in_bias
        joined = reduced_backward(low(joined))
        queries = joined[:, :, :width].reshape(length, group_rows, HEADS, HEAD_DIM)
        keys_part = joined[:, :, width:2 * width].reshape(length, group_rows, HEADS, HEAD_DIM)
        values_part = joined[:, :, 2 * width:].reshape(length, group_rows, HEADS, HEAD_DIM)
        scores = reduced_backward(gain_product('qrhd,krhd->rhqk', queries, keys_part) * SCORE_SCALE)
        scores = jnp.where(same_image[:, None], scores, MASK_FILL)
        probabilities = low(jax.nn.softmax(scores, axis=-1))
        context = gain_product('rhqk,krhd->qrhd', probabilities, values_part).reshape(length, group_rows, width)
        context = reduced_backward(low(context))
        attn = reduced_backward(gain_product('trc,cd->trd', context, proj_w[layer_position])) + bias_row_block[layer_position, 3]
        middle_residual = residual_rows + keep_attn * attn / KEEP_RATE
        second_normed_rows = low(layer_norm(middle_residual, gain_row_block[layer_position, 1], bias_row_block[layer_position, 4]))
        hidden_before_gelu = reduced_backward(gain_product('klz,zg->klg', second_normed_rows, expand_weight[layer_position]) + expand_bias[layer_position])
        hidden_activated = low(jax.nn.gelu(hidden_before_gelu, approximate=False))
        feedforward_block = reduced_backward(gain_product('zjl,lc->zjc', hidden_activated, contract_weight[layer_position])) + bias_row_block[layer_position, 5]
        residual_rows = middle_residual + keep_mlp * feedforward_block / KEEP_RATE
    return residual_rows

def forward(residual_rows, qkv_w, proj_w, expand_weight, contract_weight, gain_row_block, bias_row_block, expand_bias, segments, keep_flags):
    groups = NROWS
    width = residual_rows.shape[2]
    pieces = residual_rows.reshape(ROW_LEN, groups, 1, width).transpose(1, 0, 2, 3)
    seg_groups = segments.reshape(groups, 1, ROW_LEN)
    flag_groups = keep_flags.reshape(LAYERS, 2, groups, 1, SEGS).transpose(2, 0, 1, 3, 4).astype(jnp.float32)
    params = (qkv_w, proj_w, expand_weight, contract_weight, gain_row_block, bias_row_block, expand_bias)
    checked = jax.checkpoint(run_group)

    def step(carry, item):
        return (carry, checked(item[0], item[1], item[2], params))
    _, outputs = lax.scan(step, None, (pieces, seg_groups, flag_groups))
    return outputs.transpose(1, 0, 2, 3).reshape(ROW_LEN, NROWS, width)

def reference(block_input, cotangent, qkv_weight, proj_weight, fc1_weight, fc2_weight, norm_gains, biases, fc1_bias, segments, keep_flags):

    def wrapped(residual_rows, qkv_w, proj_w, expand_weight, contract_weight, gain_row_block, bias_row_block, expand_bias):
        return forward(residual_rows, qkv_w, proj_w, expand_weight, contract_weight, gain_row_block, bias_row_block, expand_bias, segments, keep_flags)
    output, pullback = jax.vjp(wrapped, block_input.astype(jnp.float32), qkv_weight.astype(jnp.float32), proj_weight.astype(jnp.float32), fc1_weight.astype(jnp.float32), fc2_weight.astype(jnp.float32), norm_gains.astype(jnp.float32), biases.astype(jnp.float32), fc1_bias.astype(jnp.float32))
    grads = pullback(cotangent.astype(jnp.float32))
    return (output, grads[0], grads[1], grads[2], grads[3], grads[4], grads[5], grads[6], grads[7])
```

```python
import math

import jax
import jax.numpy as jnp
from jax import lax
from jax.sharding import PartitionSpec as P

HEAD_DIM = 64
LAYERS = 2
SEGS = 8

NORM_EPS = 1e-06
KEEP_RATE = 0.9
SCORE_SCALE = 0.125
MASK_FILL = -1e30
INV_SQRT_TWO = 1.0 / math.sqrt(2.0)
INV_SQRT_TWO_PI = 1.0 / math.sqrt(2.0 * math.pi)


def apply_layer_norm(residual_rows):
    center = residual_rows - jnp.mean(residual_rows, axis=-1, keepdims=True)
    spread = jnp.mean(center * center, axis=-1, keepdims=True)
    inverse_deviation = lax.rsqrt(spread + NORM_EPS)
    return (center * inverse_deviation, inverse_deviation)


def norm_backward(normed_gradient, centered_unit, inverse_deviation, norm_gain):
    scaled_rows = normed_gradient * norm_gain
    return inverse_deviation * (
        scaled_rows
        - jnp.mean(scaled_rows, axis=-1, keepdims=True)
        - centered_unit * jnp.mean(scaled_rows * centered_unit, axis=-1, keepdims=True)
    )


def cumulative(u):
    return 0.5 * (1.0 + lax.erf(u * INV_SQRT_TWO))


def gelu_slope(u):
    return cumulative(u) + u * jnp.exp(-0.5 * u * u) * INV_SQRT_TWO_PI


def mul(a, b, dims):
    return lax.dot_general(a, b, (dims, ((), ())), preferred_element_type=jnp.float32)


def gather_packed(shard):
    return lax.all_gather(shard, "rows", axis=0, tiled=True)


def scatter_packed(partial):
    return lax.psum_scatter(partial, "rows", scatter_dimension=0, tiled=True)


def per_device(
    block_input,
    cotangent,
    qkv_weight,
    proj_weight,
    fc1_weight,
    fc2_weight,
    norm_gains,
    biases,
    fc1_bias,
    segments,
    keep_flags,
):
    local_len, row_count, width = block_input.shape
    assert row_count == 1
    tp_rank = lax.axis_index("tp")
    tp_size = lax.axis_size("tp")
    full_len = local_len * tp_size
    shard_rows = qkv_weight.shape[1]
    head_cols = qkv_weight.shape[3]
    ff_cols = fc1_weight.shape[2]
    head_count = head_cols // HEAD_DIM
    qkv_end = 3 * head_cols
    proj_end = qkv_end + head_cols
    fc1_end = proj_end + ff_cols
    bf16 = jnp.bfloat16
    f32 = jnp.float32

    segment_row = segments[0]
    same_image = segment_row[:, None] == segment_row[None, :]
    local_segments = lax.dynamic_slice_in_dim(segment_row, tp_rank * local_len, local_len, 0)
    member = (
        local_segments[:, None] == jnp.arange(SEGS, dtype=jnp.int32)[None, :]
    ).astype(f32)

    def token_keep(keep_row):
        return jnp.sum(member * keep_row.astype(f32), axis=1, keepdims=True)

    def place(part_grad, total_len):
        return lax.dynamic_update_slice_in_dim(
            jnp.zeros((total_len,), f32), part_grad, tp_rank * part_grad.shape[0], 0
        )

    def gather_positions(local_rows):
        return lax.all_gather(local_rows, "tp", axis=0, tiled=True)

    def scatter_positions(partial):
        if tp_size == 2:
            halves = partial.reshape(2, local_len, width)
            away = lax.dynamic_index_in_dim(halves, 1 - tp_rank, 0, keepdims=False)
            mine = lax.dynamic_index_in_dim(halves, tp_rank, 0, keepdims=False)
            arrived = lax.ppermute(away, "tp", [(0, 1), (1, 0)])
            return mine.astype(f32) + arrived.astype(f32)
        return lax.psum_scatter(partial, "tp", scatter_dimension=0, tiled=True).astype(f32)

    packed_full = [
        gather_packed(
            jnp.concatenate(
                [
                    qkv_weight[layer].reshape(shard_rows, qkv_end).astype(bf16),
                    proj_weight[layer].T.astype(bf16),
                    fc1_weight[layer].astype(bf16),
                    fc2_weight[layer].T.astype(bf16),
                ],
                axis=1,
            )
        )
        for layer in range(LAYERS)
    ]
    vector_parts = [norm_gains, biases, fc1_bias[:, None, :]]
    vector_full = lax.all_gather(
        jnp.concatenate([part.reshape(-1) for part in vector_parts]),
        ("rows", "tp"),
        axis=0,
        tiled=False,
    )
    full_vectors = []
    first = 0
    for part in vector_parts:
        taken = vector_full[:, first : first + part.size].reshape((-1,) + part.shape)
        first += part.size
        full_vectors.append(jnp.moveaxis(taken, 0, 2).reshape(part.shape[0], part.shape[1], -1))
    gains_full, biases_full, fc1_bias_full = full_vectors

    def heads(rows):
        return jnp.transpose(rows.reshape(full_len, head_count, HEAD_DIM), (1, 0, 2))

    def unheads(by_head):
        return jnp.transpose(by_head, (1, 0, 2)).reshape(full_len, head_cols)

    def head_mul(a, b, dims):
        return lax.dot_general(a, b, (dims, ((0,), (0,))), preferred_element_type=f32)

    def attention_scores(queries, keys):
        scores = head_mul(queries, keys, ((2,), (2,))) * SCORE_SCALE
        return jnp.where(same_image[None], scores, MASK_FILL)

    stream = block_input[:, 0]
    saved = []
    for layer in range(LAYERS):
        packed = packed_full[layer]
        w_qkv = packed[:, :qkv_end]
        w_proj = packed[:, qkv_end:proj_end]
        w_fc1 = packed[:, proj_end:fc1_end]
        w_fc2 = packed[:, fc1_end:]
        gain = gains_full[layer]
        bias = biases_full[layer]
        in_bias = jnp.concatenate(
            [
                lax.dynamic_slice_in_dim(bias[1], tp_rank * head_cols, head_cols, 0),
                jnp.zeros((head_cols,), f32),
                lax.dynamic_slice_in_dim(bias[2], tp_rank * head_cols, head_cols, 0),
            ]
        )
        up_bias = lax.dynamic_slice_in_dim(fc1_bias_full[layer, 0], tp_rank * ff_cols, ff_cols, 0)
        keep_attn = token_keep(keep_flags[layer, 0])
        keep_mlp = token_keep(keep_flags[layer, 1])
        xhat_one, rstd_one = apply_layer_norm(stream)
        normed_one = gather_positions((xhat_one * gain[0] + bias[0]).astype(bf16))
        joined = (mul(normed_one, w_qkv, ((1,), (0,))) + in_bias).astype(bf16)
        queries = heads(joined[:, :head_cols])
        keys = heads(joined[:, head_cols : 2 * head_cols])
        values = heads(joined[:, 2 * head_cols :])
        scores = attention_scores(queries, keys)
        top = jnp.max(scores, axis=-1, keepdims=True)
        exponent = jnp.exp(scores - top)
        total = jnp.sum(exponent, axis=-1, keepdims=True)
        log_total = top + jnp.log(total)
        probs = (exponent / total).astype(bf16)
        context = unheads(head_mul(probs, values, ((2,), (1,))).astype(bf16))
        attn = scatter_positions(mul(context, w_proj, ((1,), (1,))).astype(bf16)) + bias[3]
        middle = stream + keep_attn * attn / KEEP_RATE
        xhat_two, rstd_two = apply_layer_norm(middle)
        normed_two = gather_positions((xhat_two * gain[1] + bias[4]).astype(bf16))
        hidden_pre = mul(normed_two, w_fc1, ((1,), (0,))) + up_bias
        hidden = (hidden_pre * cumulative(hidden_pre)).astype(bf16)
        mlp = scatter_positions(mul(hidden, w_fc2, ((1,), (1,))).astype(bf16)) + bias[5]
        stream = middle + keep_mlp * mlp / KEEP_RATE
        saved.append(
            (
                (w_qkv, w_proj, w_fc1, w_fc2, gain, keep_attn, keep_mlp),
                (xhat_one, rstd_one, normed_one, queries, keys, values, log_total, context),
                (xhat_two, rstd_two, normed_two, hidden_pre, hidden),
            )
        )

    grad = cotangent[:, 0]
    weight_grads = [None] * LAYERS
    vector_grads = [None] * LAYERS
    for layer in reversed(range(LAYERS)):
        (w_qkv, w_proj, w_fc1, w_fc2, gain, keep_attn, keep_mlp), attn_side, mlp_side = saved[layer]
        xhat_one, rstd_one, normed_one, queries, keys, values, log_total, context = attn_side
        xhat_two, rstd_two, normed_two, hidden_pre, hidden = mlp_side
        mlp_grad = grad * keep_mlp / KEEP_RATE
        fc2_bias_grad = jnp.sum(mlp_grad, axis=0)
        mlp_low = gather_positions(mlp_grad.astype(bf16))
        hidden_grad = mul(mlp_low, w_fc2, ((1,), (0,)))
        pre_grad = (hidden_grad * gelu_slope(hidden_pre)).astype(bf16)
        fc1_bias_grad = jnp.sum(pre_grad.astype(f32), axis=0)
        two_grad = scatter_positions(mul(pre_grad, w_fc1, ((1,), (1,))).astype(bf16))
        gain_two_grad = jnp.sum(two_grad * xhat_two, axis=0)
        shift_two_grad = jnp.sum(two_grad, axis=0)
        middle_grad = grad + norm_backward(two_grad, xhat_two, rstd_two, gain[1])
        attn_grad = middle_grad * keep_attn / KEEP_RATE
        proj_bias_grad = jnp.sum(attn_grad, axis=0)
        attn_low = gather_positions(attn_grad.astype(bf16))
        context_low = heads(mul(attn_low, w_proj, ((1,), (0,))).astype(bf16))
        scores = attention_scores(queries, keys)
        probabilities = jnp.exp(scores - log_total)
        value_grad = head_mul(probabilities.astype(bf16), context_low, ((1,), (1,)))
        prob_grad = head_mul(context_low, values, ((2,), (2,)))
        row_delta = jnp.sum(prob_grad * probabilities, axis=-1, keepdims=True)
        score_grad = (probabilities * (prob_grad - row_delta)).astype(bf16)
        query_grad = head_mul(score_grad, keys, ((2,), (1,))) * SCORE_SCALE
        key_grad = head_mul(score_grad, queries, ((1,), (1,))) * SCORE_SCALE
        joined_grad = jnp.concatenate(
            [unheads(part.astype(bf16)) for part in (query_grad, key_grad, value_grad)], axis=1
        )
        in_bias_grad = jnp.sum(joined_grad.astype(f32), axis=0)
        one_grad = scatter_positions(mul(joined_grad, w_qkv, ((1,), (1,))).astype(bf16))
        gain_one_grad = jnp.sum(one_grad * xhat_one, axis=0)
        shift_one_grad = jnp.sum(one_grad, axis=0)
        grad = middle_grad + norm_backward(one_grad, xhat_one, rstd_one, gain[0])
        weight_grads[layer] = scatter_packed(
            jnp.concatenate(
                [
                    mul(normed_one, joined_grad, ((0,), (0,))).astype(bf16),
                    mul(attn_low, context, ((0,), (0,))).astype(bf16),
                    mul(normed_two, pre_grad, ((0,), (0,))).astype(bf16),
                    mul(mlp_low, hidden, ((0,), (0,))).astype(bf16),
                ],
                axis=1,
            )
        )
        vector_grads[layer] = [
            gain_one_grad,
            gain_two_grad,
            shift_one_grad,
            place(in_bias_grad[:head_cols], width),
            place(in_bias_grad[2 * head_cols :], width),
            proj_bias_grad,
            shift_two_grad,
            fc2_bias_grad,
            place(fc1_bias_grad, ff_cols * tp_size),
        ]

    shares = tp_size * lax.axis_size("rows")
    vector_sum = lax.psum_scatter(
        jnp.concatenate(
            [part.reshape(shares, -1) for layer in vector_grads for part in layer], axis=1
        ),
        ("rows", "tp"),
        scatter_dimension=0,
        tiled=True,
    ).reshape(LAYERS, -1)
    part_len = width // shares
    weight_sum = jnp.stack(weight_grads).astype(f32)
    return (
        stream[:, None],
        grad[:, None],
        weight_sum[:, :, :qkv_end].reshape(LAYERS, shard_rows, 3, head_cols),
        jnp.transpose(weight_sum[:, :, qkv_end:proj_end], (0, 2, 1)),
        weight_sum[:, :, proj_end:fc1_end],
        jnp.transpose(weight_sum[:, :, fc1_end:], (0, 2, 1)),
        vector_sum[:, : 2 * part_len].reshape(LAYERS, 2, part_len),
        vector_sum[:, 2 * part_len : 8 * part_len].reshape(LAYERS, 6, part_len),
        vector_sum[:, 8 * part_len :],
    )


def solution(mesh):
    placed = (
        P("tp", "rows", None),
        P("tp", "rows", None),
        P(None, "rows", None, "tp"),
        P(None, "tp", "rows"),
        P(None, "rows", "tp"),
        P(None, "tp", "rows"),
        P(None, None, ("rows", "tp")),
        P(None, None, ("rows", "tp")),
        P(None, ("rows", "tp")),
        P("rows", None),
        P(None, None, "rows", None),
    )
    return jax.shard_map(
        per_device,
        mesh=mesh,
        in_specs=placed,
        out_specs=placed[:2] + placed[2:9],
        check_vma=False,
    )
```

```python
import functools
import math

import jax
import jax.numpy as jnp
from jax import lax
from jax.experimental import pallas as pl
from jax.experimental.pallas import tpu as pltpu
from jax.sharding import PartitionSpec as P

MESH = pl.DeviceIdType.MESH
LANES = 128
GATHER_ORDERS = ("zyx", "zxy", "xyz")
HEAD_DIM = 64
LAYERS = 2
SEGS = 8

NORM_EPS = 1e-06
KEEP_RATE = 0.9
SCORE_SCALE = 0.125
MASK_FILL = -1e30
INV_SQRT_TWO = 1.0 / math.sqrt(2.0)
INV_SQRT_TWO_PI = 1.0 / math.sqrt(2.0 * math.pi)


def apply_layer_norm(residual_rows):
    center = residual_rows - jnp.mean(residual_rows, axis=-1, keepdims=True)
    spread = jnp.mean(center * center, axis=-1, keepdims=True)
    inverse_deviation = lax.rsqrt(spread + NORM_EPS)
    return (center * inverse_deviation, inverse_deviation)


def norm_backward(normed_gradient, centered_unit, inverse_deviation, norm_gain):
    scaled_rows = normed_gradient * norm_gain
    return inverse_deviation * (
        scaled_rows
        - jnp.mean(scaled_rows, axis=-1, keepdims=True)
        - centered_unit * jnp.mean(scaled_rows * centered_unit, axis=-1, keepdims=True)
    )


def cumulative(u):
    return 0.5 * (1.0 + lax.erf(u * INV_SQRT_TWO))


def gelu_slope(u):
    return cumulative(u) + u * jnp.exp(-0.5 * u * u) * INV_SQRT_TWO_PI


def mul(a, b, dims):
    return lax.dot_general(a, b, (dims, ((), ())), preferred_element_type=jnp.float32)


def split_columns(total):
    groups = total // LANES
    first = groups * 14 // 36
    return (
        (0, first * LANES),
        (first * LANES, first * LANES),
        (2 * first * LANES, (groups - 2 * first) * LANES),
    )


def places(nz):
    me = lax.axis_index("rows")
    px = lax.rem(me, 2)
    py = lax.rem(lax.div(me, 2), 2)
    pz = lax.div(me, 4)
    hops = {
        "x": me + 1 - 2 * px,
        "y": me + 2 - 4 * py,
        "u": lax.min(me + 4, 4 * nz - 1),
        "d": lax.max(me - 4, 0),
    }
    return me, px, py, pz, hops


def guarded(cond, act):
    if cond is None:
        act()
    else:
        pl.when(cond)(act)


def both(a, b):
    if a is None:
        return b
    if b is None:
        return a
    return jnp.logical_and(a, b)


def greet(nz, pz, hops, tp, with_tp):
    barrier = pltpu.get_barrier_semaphore()
    ends = {"x": None, "y": None, "u": pz < nz - 1, "d": pz > 0}
    for name, cond in ends.items():
        guarded(
            cond,
            lambda name=name: pl.semaphore_signal(
                barrier, inc=1, device_id=(hops[name], tp), device_id_type=MESH
            ),
        )
    waits = 2
    if with_tp:
        pl.semaphore_signal(
            barrier, inc=1, device_id=(lax.axis_index("rows"), 1 - tp), device_id_type=MESH
        )
        waits = 3
    waits = waits + lax.min(pz, 1) + lax.min(nz - 1 - pz, 1)
    pl.semaphore_wait(barrier, waits)
    return ends


def gather_plan(order, nz):
    found = []
    for rx in (0, 1):
        for ry in (0, 1):
            for rz in range(1 - nz, nz):
                rel = {"x": rx, "y": ry, "z": rz}
                differing = [i for i, dim in enumerate(order) if rel[dim]]
                last = differing[-1] if differing else -1
                sends = []
                if last >= 0 and order[last] == "z":
                    sends.append("u" if rz < 0 else "d")
                for dim in order[last + 1 :]:
                    sends.extend("ud" if dim == "z" else dim)
                found.append((last + 1, abs(rz), rx + ry, rx, ry, rz, tuple(sends)))
    return sorted(found)


def gather_kernel(nz, layers, rows, cols, shard, vec, full, vec_full, own_sem, recv, send):
    me, px, py, pz, hops = places(nz)
    tp = lax.axis_index("tp")
    n = 4 * nz
    spans = split_columns(cols)
    names = "xyud"
    ends = greet(nz, pz, hops, tp, True)

    def origin(rx, ry, rz):
        return me + rx * (1 - 2 * px) + ry * 2 * (1 - 2 * py) + 4 * rz

    def block(layer, color, o):
        start = pl.multiple_of((layer * n + o) * rows, 16)
        return full.at[pl.ds(start, rows), pl.ds(*spans[color])]

    def copy(layer, color, o, name, own):
        if color == 3:
            src = vec_full.at[o]
            dst = vec_full.at[o]
        else:
            dst = block(layer, color, o)
            src = dst
            if own:
                start = pl.multiple_of(layer * rows, 16)
                src = shard.at[pl.ds(start, rows), pl.ds(*spans[color])]
        return pltpu.make_async_remote_copy(
            src_ref=src,
            dst_ref=dst,
            send_sem=send.at[layer, color, names.index(name), o],
            recv_sem=recv.at[layer, color, o],
            device_id=(hops[name], tp),
            device_id_type=MESH,
        )

    keep = pltpu.make_async_copy(vec, vec_full.at[me, tp], own_sem.at[0])
    keep.start()
    swap = pltpu.make_async_remote_copy(
        src_ref=vec,
        dst_ref=vec_full.at[me, tp],
        send_sem=own_sem.at[1],
        recv_sem=own_sem.at[2],
        device_id=(me, 1 - tp),
        device_id_type=MESH,
    )
    swap.start()
    plans = [gather_plan(order, nz) for order in GATHER_ORDERS + ("xyz",)]

    def visit(layer, color, item, waiting):
        _, _, _, rx, ry, rz, sends = item
        o = origin(rx, ry, rz)
        own = (rx, ry, rz) == (0, 0, 0)
        valid = None if rz == 0 else jnp.logical_and(pz + rz >= 0, pz + rz < nz)

        def act():
            if not waiting and not own:
                name = "x"
                copy(layer, color, o, name, False).wait_recv()
            for name in sends:

                def go(name=name):
                    c = copy(layer, color, o, name, own)
                    if waiting:
                        c.wait_send()
                    else:
                        c.start()

                guarded(ends[name], go)

        guarded(valid, act)

    def own_place(layer):
        src = shard.at[pl.ds(pl.multiple_of(layer * rows, 16), rows), :]
        dst = full.at[pl.ds(pl.multiple_of((layer * n + me) * rows, 16), rows), :]
        return pltpu.make_async_copy(src, dst, own_sem.at[3 + layer])

    for phase in range(4):
        stacks = [[item for item in plan if item[0] == phase] for plan in plans]

        def step(layer, carry):
            for i in range(max(len(s) for s in stacks[:3])):
                for color in range(3):
                    if i < len(stacks[color]):
                        visit(layer, color, stacks[color][i], False)
            return carry

        lax.fori_loop(0, layers, step, 0)
        if phase == 0:
            lax.fori_loop(0, layers, lambda layer, c: (own_place(layer).start(), c)[1], 0)
            keep.wait()
            swap.wait()
        for item in stacks[3]:
            visit(0, 3, item, False)

    def finish(layer, carry):
        for color in range(3):
            for item in plans[color]:
                visit(layer, color, item, True)
        own_place(layer).wait()
        return carry

    lax.fori_loop(0, layers, finish, 0)
    for item in plans[3]:
        visit(0, 3, item, True)


def gather_rows(shards, vec, nz):
    layers, rows, cols = shards.shape
    n = 4 * nz
    any_space = pl.BlockSpec(memory_space=pl.ANY)
    vmem = pl.BlockSpec(memory_space=pltpu.VMEM)
    full, vec_full = pl.pallas_call(
        functools.partial(gather_kernel, nz, layers, rows, cols),
        out_shape=(
            jax.ShapeDtypeStruct((layers * n * rows, cols), shards.dtype),
            jax.ShapeDtypeStruct((n, 2) + vec.shape, vec.dtype),
        ),
        in_specs=[vmem, vmem],
        out_specs=(any_space, any_space),
        scratch_shapes=[
            pltpu.SemaphoreType.DMA((3 + layers,)),
            pltpu.SemaphoreType.DMA((layers, 4, n)),
            pltpu.SemaphoreType.DMA((layers, 4, 4, n)),
        ],
        compiler_params=pltpu.CompilerParams(
            collective_id=0, has_side_effects=True, vmem_limit_bytes=8 * 1024 * 1024
        ),
        name="gather_rows",
    )(shards.reshape(layers * rows, cols), vec)
    return full.reshape(layers, n * rows, cols), vec_full


def sum_kernel(nz, layers, rows, cols, part, out, ra, rb, rc, ry_c, rx_c, sc, send, recv):
    me, px, py, pz, hops = places(nz)
    tp = lax.axis_index("tp")
    n = 4 * nz
    spans = split_columns(cols)
    ends = greet(nz, pz, hops, tp, False)
    base = (0, 5 * nz, 10 * nz)
    pools = (ra, rb)
    coord = {"x": px, "y": py}
    stride = {"x": 1, "y": 2}
    zs = []
    for k in range((nz + 1) // 2):
        zs.extend([nz - 1 - k, k] if nz - 1 - k != k else [k])

    def mine(layer, o, color, count=1):
        start = pl.multiple_of((layer * n + o) * rows, 16)
        return part.at[pl.ds(start, count * rows), pl.ds(*spans[color])]

    def copy(src, dst, layer, index, name):
        return pltpu.make_async_remote_copy(
            src_ref=src,
            dst_ref=dst,
            send_sem=send.at[layer, index],
            recv_sem=recv.at[layer, index],
            device_id=(hops[name], tp),
            device_id_type=MESH,
        )

    def add(dst, sources, count=rows):
        def chunk(i, carry):
            at = pl.ds(pl.multiple_of(i * 16, 16), 16)
            total = sources[0][at, :].astype(jnp.float32)
            for s in sources[1:]:
                total = total + s[at, :].astype(jnp.float32)
            dst[at, :] = total.astype(dst.dtype)
            return carry

        lax.fori_loop(0, count // 16, chunk, 0)

    def over_layers(act):
        lax.fori_loop(0, layers, lambda layer, c: (act(layer), c)[1], 0)

    dims = (("x", "y"), ("y", "x"))

    def dest(color, flip_one, flip_two, z):
        d1, d2 = dims[color]
        c1 = coord[d1] if not flip_one else 1 - coord[d1]
        c2 = coord[d2] if not flip_two else 1 - coord[d2]
        return 4 * z + stride[d1] * c1 + stride[d2] * c2

    def hop_one(layer, color, flip_two, z):
        slot = flip_two * nz + z
        dst = pools[color].at[layer, slot]
        return copy(
            mine(layer, dest(color, 1, flip_two, z), color),
            dst,
            layer,
            base[color] + slot,
            dims[color][0],
        )

    def hop_two(layer, color, z):
        pool = pools[color]
        slot = 2 * nz + z
        return copy(
            pool.at[layer, nz + z], pool.at[layer, slot], layer, base[color] + slot, dims[color][1]
        )

    def line(layer, color, z, name):
        pool = pools[color]
        slot = (3 if name == "u" else 4) * nz + z
        return copy(
            pool.at[layer, 2 * nz + z], pool.at[layer, slot], layer, base[color] + slot, name
        )

    def line_c(layer, z, name, direct):
        slot = (0 if name == "u" else nz) + z
        dst = rc.at[layer, slot]
        src = mine(layer, 4 * z, 2, 4) if direct else dst
        return copy(src, dst, layer, base[2] + slot, name)

    def swap_y(layer):
        src = sc.at[layer, pl.ds(pl.multiple_of((1 - py) * 2 * rows, 16), 2 * rows), :]
        return copy(src, ry_c.at[layer], layer, base[2] + 2 * nz, "y")

    def swap_x(layer):
        src = ry_c.at[layer, pl.ds(pl.multiple_of((1 - px) * rows, 16), rows), :]
        return copy(src, rx_c.at[layer], layer, base[2] + 2 * nz + 1, "x")

    def start_all(layer):
        for z in zs:
            for color in range(2):
                hop_one(layer, color, 1, z).start()
            if z > 0:
                pl.when(pz == 0)(lambda z=z: line_c(layer, z, "u", True).start())
            if z < nz - 1:
                pl.when(pz == nz - 1)(lambda z=z: line_c(layer, z, "d", True).start())
        for z in zs:
            for color in range(2):
                hop_one(layer, color, 0, z).start()

    def relay_c(layer, z):
        if z > 1:

            @pl.when(jnp.logical_and(pz > 0, pz < z))
            def _():
                c = line_c(layer, z, "u", False)
                c.wait_recv()
                add(rc.at[layer, z], (mine(layer, 4 * z, 2, 4), rc.at[layer, z]), 4 * rows)
                c.start()

        if z < nz - 2:

            @pl.when(jnp.logical_and(pz < nz - 1, pz > z))
            def _():
                c = line_c(layer, z, "d", False)
                c.wait_recv()
                at = rc.at[layer, nz + z]
                add(at, (mine(layer, 4 * z, 2, 4), at), 4 * rows)
                c.start()

    def second(layer):
        for z in zs:
            for color in range(2):
                hop_one(layer, color, 1, z).wait_recv()
                at = pools[color].at[layer, nz + z]
                add(at, (mine(layer, dest(color, 0, 1, z), color), at))
                hop_two(layer, color, z).start()
            relay_c(layer, z)

    def settle_c(layer):
        up = line_c(layer, pz, "u", False)
        down = line_c(layer, pz, "d", False)
        own = mine(layer, 4 * pz, 2, 4)
        from_up = rc.at[layer, pz]
        from_down = rc.at[layer, nz + pz]
        target = sc.at[layer]

        @pl.when(pz == 0)
        def _():
            down.wait_recv()
            add(target, (own, from_down), 4 * rows)

        @pl.when(pz == nz - 1)
        def _():
            up.wait_recv()
            add(target, (own, from_up), 4 * rows)

        @pl.when(jnp.logical_and(pz > 0, pz < nz - 1))
        def _():
            down.wait_recv()
            up.wait_recv()
            add(target, (own, from_up, from_down), 4 * rows)

        swap_y(layer).start()

    def third(layer):
        for z in zs:
            for color in range(2):
                pool = pools[color]
                hop_one(layer, color, 0, z).wait_recv()
                hop_two(layer, color, z).wait_recv()
                at = pool.at[layer, 2 * nz + z]
                add(at, (mine(layer, dest(color, 0, 0, z), color), pool.at[layer, z], at))
                pl.when(jnp.logical_and(pz == 0, z > pz))(
                    lambda c=color, z=z: line(layer, c, z, "u").start()
                )
                pl.when(jnp.logical_and(pz == nz - 1, z < pz))(
                    lambda c=color, z=z: line(layer, c, z, "d").start()
                )

    def relay(layer):
        for z in zs:
            for color in range(2):
                pool = pools[color]
                at = pool.at[layer, 2 * nz + z]

                @pl.when(jnp.logical_and(pz > 0, pz < z))
                def _():
                    c = line(layer, color, z, "u")
                    c.wait_recv()
                    add(at, (at, pool.at[layer, 3 * nz + z]))
                    c.start()

                @pl.when(jnp.logical_and(pz < nz - 1, pz > z))
                def _():
                    c = line(layer, color, z, "d")
                    c.wait_recv()
                    add(at, (at, pool.at[layer, 4 * nz + z]))
                    c.start()

    def out_at(layer, color):
        return out.at[pl.ds(pl.multiple_of(layer * rows, 16), rows), pl.ds(*spans[color])]

    def x_c(layer):
        swap_y(layer).wait_recv()
        own = sc.at[layer, pl.ds(pl.multiple_of(py * 2 * rows, 16), 2 * rows), :]
        add(ry_c.at[layer], (own, ry_c.at[layer]), 2 * rows)
        swap_x(layer).start()

    def final(layer):
        for color in range(2):
            pool = pools[color]
            up = line(layer, color, pz, "u")
            down = line(layer, color, pz, "d")
            own = pool.at[layer, 2 * nz + pz]
            from_up = pool.at[layer, 3 * nz + pz]
            from_down = pool.at[layer, 4 * nz + pz]
            target = out_at(layer, color)

            @pl.when(pz == 0)
            def _():
                down.wait_recv()
                add(target, (own, from_down))

            @pl.when(pz == nz - 1)
            def _():
                up.wait_recv()
                add(target, (own, from_up))

            @pl.when(jnp.logical_and(pz > 0, pz < nz - 1))
            def _():
                down.wait_recv()
                up.wait_recv()
                add(target, (own, from_up, from_down))

        swap_x(layer).wait_recv()
        own = ry_c.at[layer, pl.ds(pl.multiple_of(px * rows, 16), rows), :]
        add(out_at(layer, 2), (own, rx_c.at[layer]))

    def drain(layer):
        for z in zs:
            for color in range(2):
                hop_one(layer, color, 1, z).wait_send()
                hop_one(layer, color, 0, z).wait_send()
                hop_two(layer, color, z).wait_send()
                pl.when(pz < z)(lambda c=color, z=z: line(layer, c, z, "u").wait_send())
                pl.when(pz > z)(lambda c=color, z=z: line(layer, c, z, "d").wait_send())
            pl.when(pz < z)(lambda z=z: line_c(layer, z, "u", False).wait_send())
            pl.when(pz > z)(lambda z=z: line_c(layer, z, "d", False).wait_send())
        swap_y(layer).wait_send()
        swap_x(layer).wait_send()

    for act in (start_all, second, settle_c, third, x_c, relay, final, drain):
        over_layers(act)


def sum_rows(parts, nz):
    layers, depth, cols = parts.shape
    n = 4 * nz
    rows = depth // n
    spans = split_columns(cols)
    vmem = pl.BlockSpec(memory_space=pltpu.VMEM)
    dt = parts.dtype
    count = 12 * nz + 2
    out = pl.pallas_call(
        functools.partial(sum_kernel, nz, layers, rows, cols),
        out_shape=jax.ShapeDtypeStruct((layers * rows, cols), jnp.float32),
        in_specs=[vmem],
        out_specs=vmem,
        scratch_shapes=[
            pltpu.VMEM((layers, 5 * nz, rows, spans[0][1]), dt),
            pltpu.VMEM((layers, 5 * nz, rows, spans[1][1]), dt),
            pltpu.VMEM((layers, 2 * nz, 4 * rows, spans[2][1]), dt),
            pltpu.VMEM((layers, 2 * rows, spans[2][1]), dt),
            pltpu.VMEM((layers, rows, spans[2][1]), dt),
            pltpu.VMEM((layers, 4 * rows, spans[2][1]), dt),
            pltpu.SemaphoreType.DMA((layers, count)),
            pltpu.SemaphoreType.DMA((layers, count)),
        ],
        compiler_params=pltpu.CompilerParams(
            collective_id=1, has_side_effects=True, vmem_limit_bytes=60 * 1024 * 1024
        ),
        name="sum_rows",
    )(parts.reshape(layers * depth, cols))
    return out.reshape(layers, rows, cols)


def pair_sum(rows, tp_rank):
    layers, depth, cols = rows.shape
    halves = rows.reshape(layers, 2, depth // 2, cols)
    away = lax.dynamic_index_in_dim(halves, 1 - tp_rank, 1, keepdims=False)
    mine = lax.dynamic_index_in_dim(halves, tp_rank, 1, keepdims=False)
    return mine + lax.ppermute(away, "tp", [(0, 1), (1, 0)])


def per_device(
    block_input,
    cotangent,
    qkv_weight,
    proj_weight,
    fc1_weight,
    fc2_weight,
    norm_gains,
    biases,
    fc1_bias,
    segments,
    keep_flags,
):
    local_len, row_count, width = block_input.shape
    assert row_count == 1
    tp_rank = lax.axis_index("tp")
    tp_size = lax.axis_size("tp")
    full_len = local_len * tp_size
    shard_rows = qkv_weight.shape[1]
    head_cols = qkv_weight.shape[3]
    ff_cols = fc1_weight.shape[2]
    head_count = head_cols // HEAD_DIM
    qkv_end = 3 * head_cols
    proj_end = qkv_end + head_cols
    fc1_end = proj_end + ff_cols
    bf16 = jnp.bfloat16
    f32 = jnp.float32

    segment_row = segments[0]
    same_image = segment_row[:, None] == segment_row[None, :]
    local_segments = lax.dynamic_slice_in_dim(segment_row, tp_rank * local_len, local_len, 0)
    member = (
        local_segments[:, None] == jnp.arange(SEGS, dtype=jnp.int32)[None, :]
    ).astype(f32)

    def token_keep(keep_row):
        return jnp.sum(member * keep_row.astype(f32), axis=1, keepdims=True)

    def place(part_grad, total_len):
        return lax.dynamic_update_slice_in_dim(
            jnp.zeros((total_len,), f32), part_grad, tp_rank * part_grad.shape[0], 0
        )

    def gather_positions(local_rows):
        return lax.all_gather(local_rows, "tp", axis=0, tiled=True)

    def scatter_positions(partial):
        if tp_size == 2:
            halves = partial.reshape(2, local_len, width)
            away = lax.dynamic_index_in_dim(halves, 1 - tp_rank, 0, keepdims=False)
            mine = lax.dynamic_index_in_dim(halves, tp_rank, 0, keepdims=False)
            arrived = lax.ppermute(away, "tp", [(0, 1), (1, 0)])
            return mine.astype(f32) + arrived.astype(f32)
        return lax.psum_scatter(partial, "tp", scatter_dimension=0, tiled=True).astype(f32)

    row_devices = lax.axis_size("rows")
    own_kernels = shard_rows % 16 == 0 and row_devices % 4 == 0 and tp_size == 2
    shards = jnp.stack(
        [
            jnp.concatenate(
                [
                    qkv_weight[layer].reshape(shard_rows, qkv_end).astype(bf16),
                    proj_weight[layer].T.astype(bf16),
                    fc1_weight[layer].astype(bf16),
                    fc2_weight[layer].T.astype(bf16),
                ],
                axis=1,
            )
            for layer in range(LAYERS)
        ]
    )
    vector_parts = [norm_gains, biases, fc1_bias[:, None, :]]
    vector_flat = jnp.concatenate([part.reshape(-1) for part in vector_parts])
    if own_kernels:
        filled = -(-vector_flat.size // (8 * LANES)) * 8 * LANES
        packed_full, vector_full = gather_rows(
            shards,
            jnp.pad(vector_flat, (0, filled - vector_flat.size)).reshape(-1, LANES),
            row_devices // 4,
        )
        vector_full = vector_full.reshape(row_devices * tp_size, -1)
    else:
        packed_full = lax.all_gather(shards, "rows", axis=1, tiled=True)
        vector_full = lax.all_gather(vector_flat, ("rows", "tp"), axis=0, tiled=False)
    full_vectors = []
    first = 0
    for part in vector_parts:
        taken = vector_full[:, first : first + part.size].reshape((-1,) + part.shape)
        first += part.size
        full_vectors.append(jnp.moveaxis(taken, 0, 2).reshape(part.shape[0], part.shape[1], -1))
    gains_full, biases_full, fc1_bias_full = full_vectors

    def heads(rows):
        return jnp.transpose(rows.reshape(full_len, head_count, HEAD_DIM), (1, 0, 2))

    def unheads(by_head):
        return jnp.transpose(by_head, (1, 0, 2)).reshape(full_len, head_cols)

    def head_mul(a, b, dims):
        return lax.dot_general(a, b, (dims, ((0,), (0,))), preferred_element_type=f32)

    def attention_scores(queries, keys):
        scores = head_mul(queries, keys, ((2,), (2,))) * SCORE_SCALE
        return jnp.where(same_image[None], scores, MASK_FILL)

    stream = block_input[:, 0]
    saved = []
    for layer in range(LAYERS):
        packed = packed_full[layer]
        w_qkv = packed[:, :qkv_end]
        w_proj = packed[:, qkv_end:proj_end]
        w_fc1 = packed[:, proj_end:fc1_end]
        w_fc2 = packed[:, fc1_end:]
        gain = gains_full[layer]
        bias = biases_full[layer]
        in_bias = jnp.concatenate(
            [
                lax.dynamic_slice_in_dim(bias[1], tp_rank * head_cols, head_cols, 0),
                jnp.zeros((head_cols,), f32),
                lax.dynamic_slice_in_dim(bias[2], tp_rank * head_cols, head_cols, 0),
            ]
        )
        up_bias = lax.dynamic_slice_in_dim(fc1_bias_full[layer, 0], tp_rank * ff_cols, ff_cols, 0)
        keep_attn = token_keep(keep_flags[layer, 0])
        keep_mlp = token_keep(keep_flags[layer, 1])
        xhat_one, rstd_one = apply_layer_norm(stream)
        normed_one = gather_positions((xhat_one * gain[0] + bias[0]).astype(bf16))
        joined = (mul(normed_one, w_qkv, ((1,), (0,))) + in_bias).astype(bf16)
        queries = heads(joined[:, :head_cols])
        keys = heads(joined[:, head_cols : 2 * head_cols])
        values = heads(joined[:, 2 * head_cols :])
        scores = attention_scores(queries, keys)
        top = jnp.max(scores, axis=-1, keepdims=True)
        exponent = jnp.exp(scores - top)
        total = jnp.sum(exponent, axis=-1, keepdims=True)
        log_total = top + jnp.log(total)
        probs = (exponent / total).astype(bf16)
        context = unheads(head_mul(probs, values, ((2,), (1,))).astype(bf16))
        attn = scatter_positions(mul(context, w_proj, ((1,), (1,))).astype(bf16)) + bias[3]
        middle = stream + keep_attn * attn / KEEP_RATE
        xhat_two, rstd_two = apply_layer_norm(middle)
        normed_two = gather_positions((xhat_two * gain[1] + bias[4]).astype(bf16))
        hidden_pre = mul(normed_two, w_fc1, ((1,), (0,))) + up_bias
        hidden = (hidden_pre * cumulative(hidden_pre)).astype(bf16)
        mlp = scatter_positions(mul(hidden, w_fc2, ((1,), (1,))).astype(bf16)) + bias[5]
        stream = middle + keep_mlp * mlp / KEEP_RATE
        saved.append(
            (
                (w_qkv, w_proj, w_fc1, w_fc2, gain, keep_attn, keep_mlp),
                (xhat_one, rstd_one, normed_one, queries, keys, values, log_total, context),
                (xhat_two, rstd_two, normed_two, hidden_pre, hidden),
            )
        )

    grad = cotangent[:, 0]
    weight_grads = [None] * LAYERS
    for layer in reversed(range(LAYERS)):
        (w_qkv, w_proj, w_fc1, w_fc2, gain, keep_attn, keep_mlp), attn_side, mlp_side = saved[layer]
        xhat_one, rstd_one, normed_one, queries, keys, values, log_total, context = attn_side
        xhat_two, rstd_two, normed_two, hidden_pre, hidden = mlp_side
        mlp_grad = grad * keep_mlp / KEEP_RATE
        fc2_bias_grad = jnp.sum(mlp_grad, axis=0)
        mlp_low = gather_positions(mlp_grad.astype(bf16))
        hidden_grad = mul(mlp_low, w_fc2, ((1,), (0,)))
        pre_grad = (hidden_grad * gelu_slope(hidden_pre)).astype(bf16)
        fc1_bias_grad = jnp.sum(pre_grad.astype(f32), axis=0)
        two_grad = scatter_positions(mul(pre_grad, w_fc1, ((1,), (1,))).astype(bf16))
        gain_two_grad = jnp.sum(two_grad * xhat_two, axis=0)
        shift_two_grad = jnp.sum(two_grad, axis=0)
        middle_grad = grad + norm_backward(two_grad, xhat_two, rstd_two, gain[1])
        attn_grad = middle_grad * keep_attn / KEEP_RATE
        proj_bias_grad = jnp.sum(attn_grad, axis=0)
        attn_low = gather_positions(attn_grad.astype(bf16))
        context_low = heads(mul(attn_low, w_proj, ((1,), (0,))).astype(bf16))
        scores = attention_scores(queries, keys)
        probabilities = jnp.exp(scores - log_total)
        value_grad = head_mul(probabilities.astype(bf16), context_low, ((1,), (1,)))
        prob_grad = head_mul(context_low, values, ((2,), (2,)))
        row_delta = jnp.sum(prob_grad * probabilities, axis=-1, keepdims=True)
        score_grad = (probabilities * (prob_grad - row_delta)).astype(bf16)
        query_grad = head_mul(score_grad, keys, ((2,), (1,))) * SCORE_SCALE
        key_grad = head_mul(score_grad, queries, ((1,), (1,))) * SCORE_SCALE
        joined_grad = jnp.concatenate(
            [unheads(part.astype(bf16)) for part in (query_grad, key_grad, value_grad)], axis=1
        )
        in_bias_grad = jnp.sum(joined_grad.astype(f32), axis=0)
        one_grad = scatter_positions(mul(joined_grad, w_qkv, ((1,), (1,))).astype(bf16))
        gain_one_grad = jnp.sum(one_grad * xhat_one, axis=0)
        shift_one_grad = jnp.sum(one_grad, axis=0)
        grad = middle_grad + norm_backward(one_grad, xhat_one, rstd_one, gain[0])
        columns = [
            gain_one_grad[:, None],
            gain_two_grad[:, None],
            shift_one_grad[:, None],
            place(in_bias_grad[:head_cols], width)[:, None],
            place(in_bias_grad[2 * head_cols :], width)[:, None],
            proj_bias_grad[:, None],
            shift_two_grad[:, None],
            fc2_bias_grad[:, None],
            place(fc1_bias_grad, ff_cols * tp_size).reshape(width, -1),
        ]
        filler = LANES - sum(part.shape[1] for part in columns)
        columns.append(jnp.zeros((width, filler), f32))
        weight_grads[layer] = jnp.concatenate(
            [
                mul(normed_one, joined_grad, ((0,), (0,))).astype(bf16),
                mul(attn_low, context, ((0,), (0,))).astype(bf16),
                mul(normed_two, pre_grad, ((0,), (0,))).astype(bf16),
                mul(mlp_low, hidden, ((0,), (0,))).astype(bf16),
                jnp.concatenate(columns, axis=1).astype(bf16),
            ],
            axis=1,
        )

    partials = jnp.stack(weight_grads)
    if own_kernels:
        weight_sum = sum_rows(partials, row_devices // 4)
    else:
        weight_sum = lax.psum_scatter(
            partials, "rows", scatter_dimension=1, tiled=True
        ).astype(f32)
    fc2_end = fc1_end + ff_cols
    vector_sum = lax.psum_scatter(
        weight_sum[:, :, fc2_end:], "tp", scatter_dimension=1, tiled=True
    ) if tp_size != 2 else pair_sum(weight_sum[:, :, fc2_end:], tp_rank)
    vector_rows = jnp.transpose(vector_sum[:, :, :8], (0, 2, 1))
    return (
        stream[:, None],
        grad[:, None],
        weight_sum[:, :, :qkv_end].reshape(LAYERS, shard_rows, 3, head_cols),
        jnp.transpose(weight_sum[:, :, qkv_end:proj_end], (0, 2, 1)),
        weight_sum[:, :, proj_end:fc1_end],
        jnp.transpose(weight_sum[:, :, fc1_end:fc2_end], (0, 2, 1)),
        vector_rows[:, :2],
        vector_rows[:, 2:8],
        vector_sum[:, :, 8 : 8 + ff_cols * tp_size // width].reshape(LAYERS, -1),
    )


def solution(mesh):
    placed = (
        P("tp", "rows", None),
        P("tp", "rows", None),
        P(None, "rows", None, "tp"),
        P(None, "tp", "rows"),
        P(None, "rows", "tp"),
        P(None, "tp", "rows"),
        P(None, None, ("rows", "tp")),
        P(None, None, ("rows", "tp")),
        P(None, ("rows", "tp")),
        P("rows", None),
        P(None, None, "rows", None),
    )
    return jax.shard_map(
        per_device,
        mesh=mesh,
        in_specs=placed,
        out_specs=placed[:2] + placed[2:9],
        check_vma=False,
    )
```

```python
import functools
import math

import jax
import jax.numpy as jnp
from jax import lax
from jax.experimental import pallas as pl
from jax.experimental.pallas import tpu as pltpu
from jax.sharding import PartitionSpec as P

MESH = pl.DeviceIdType.MESH
LANES = 128
KERNEL_LAYERS = (0,)
GATHER_ORDERS = ("zyx", "zxy", "xyz")
HEAD_DIM = 64
LAYERS = 2
SEGS = 8

NORM_EPS = 1e-06
KEEP_RATE = 0.9
SCORE_SCALE = 0.125
MASK_FILL = -1e30
INV_SQRT_TWO = 1.0 / math.sqrt(2.0)
INV_SQRT_TWO_PI = 1.0 / math.sqrt(2.0 * math.pi)


def apply_layer_norm(residual_rows):
    center = residual_rows - jnp.mean(residual_rows, axis=-1, keepdims=True)
    spread = jnp.mean(center * center, axis=-1, keepdims=True)
    inverse_deviation = lax.rsqrt(spread + NORM_EPS)
    return (center * inverse_deviation, inverse_deviation)


def norm_backward(normed_gradient, centered_unit, inverse_deviation, norm_gain):
    scaled_rows = normed_gradient * norm_gain
    return inverse_deviation * (
        scaled_rows
        - jnp.mean(scaled_rows, axis=-1, keepdims=True)
        - centered_unit * jnp.mean(scaled_rows * centered_unit, axis=-1, keepdims=True)
    )


def cumulative(u):
    return 0.5 * (1.0 + lax.erf(u * INV_SQRT_TWO))


def gelu_slope(u):
    return cumulative(u) + u * jnp.exp(-0.5 * u * u) * INV_SQRT_TWO_PI


def mul(a, b, dims):
    return lax.dot_general(a, b, (dims, ((), ())), preferred_element_type=jnp.float32)


def split_columns(total):
    groups = total // LANES
    first = groups * 14 // 36
    return (
        (0, first * LANES),
        (first * LANES, first * LANES),
        (2 * first * LANES, (groups - 2 * first) * LANES),
    )


def places(nz):
    me = lax.axis_index("rows")
    px = lax.rem(me, 2)
    py = lax.rem(lax.div(me, 2), 2)
    pz = lax.div(me, 4)
    hops = {
        "x": me + 1 - 2 * px,
        "y": me + 2 - 4 * py,
        "u": lax.min(me + 4, 4 * nz - 1),
        "d": lax.max(me - 4, 0),
    }
    return me, px, py, pz, hops


def guarded(cond, act):
    if cond is None:
        act()
    else:
        pl.when(cond)(act)


def both(a, b):
    if a is None:
        return b
    if b is None:
        return a
    return jnp.logical_and(a, b)


def greet(nz, pz, hops, tp, with_tp):
    barrier = pltpu.get_barrier_semaphore()
    ends = {"x": None, "y": None, "u": pz < nz - 1, "d": pz > 0}
    for name, cond in ends.items():
        guarded(
            cond,
            lambda name=name: pl.semaphore_signal(
                barrier, inc=1, device_id=(hops[name], tp), device_id_type=MESH
            ),
        )
    waits = 2
    if with_tp:
        pl.semaphore_signal(
            barrier, inc=1, device_id=(lax.axis_index("rows"), 1 - tp), device_id_type=MESH
        )
        waits = 3
    waits = waits + lax.min(pz, 1) + lax.min(nz - 1 - pz, 1)
    pl.semaphore_wait(barrier, waits)
    return ends


def gather_plan(order, nz):
    found = []
    for rx in (0, 1):
        for ry in (0, 1):
            for rz in range(1 - nz, nz):
                rel = {"x": rx, "y": ry, "z": rz}
                differing = [i for i, dim in enumerate(order) if rel[dim]]
                last = differing[-1] if differing else -1
                sends = []
                if last >= 0 and order[last] == "z":
                    sends.append("u" if rz < 0 else "d")
                for dim in order[last + 1 :]:
                    sends.extend("ud" if dim == "z" else dim)
                found.append((last + 1, abs(rz), rx + ry, rx, ry, rz, tuple(sends)))
    return sorted(found)


def gather_kernel(nz, layers, rows, cols, shard, vec, full, vec_full, own_sem, recv, send):
    me, px, py, pz, hops = places(nz)
    tp = lax.axis_index("tp")
    n = 4 * nz
    spans = split_columns(cols)
    names = "xyud"
    ends = greet(nz, pz, hops, tp, True)

    def origin(rx, ry, rz):
        return me + rx * (1 - 2 * px) + ry * 2 * (1 - 2 * py) + 4 * rz

    def block(layer, color, o):
        start = pl.multiple_of((layer * n + o) * rows, 16)
        return full.at[pl.ds(start, rows), pl.ds(*spans[color])]

    def copy(layer, color, o, name, own):
        if color == 3:
            src = vec_full.at[o]
            dst = vec_full.at[o]
        else:
            dst = block(layer, color, o)
            src = dst
            if own:
                start = pl.multiple_of(layer * rows, 16)
                src = shard.at[pl.ds(start, rows), pl.ds(*spans[color])]
        return pltpu.make_async_remote_copy(
            src_ref=src,
            dst_ref=dst,
            send_sem=send.at[layer, color, names.index(name), o],
            recv_sem=recv.at[layer, color, o],
            device_id=(hops[name], tp),
            device_id_type=MESH,
        )

    keep = pltpu.make_async_copy(vec, vec_full.at[me, tp], own_sem.at[0])
    keep.start()
    swap = pltpu.make_async_remote_copy(
        src_ref=vec,
        dst_ref=vec_full.at[me, tp],
        send_sem=own_sem.at[1],
        recv_sem=own_sem.at[2],
        device_id=(me, 1 - tp),
        device_id_type=MESH,
    )
    swap.start()
    plans = [gather_plan(order, nz) for order in GATHER_ORDERS + ("xyz",)]

    def visit(layer, color, item, waiting):
        _, _, _, rx, ry, rz, sends = item
        o = origin(rx, ry, rz)
        own = (rx, ry, rz) == (0, 0, 0)
        valid = None if rz == 0 else jnp.logical_and(pz + rz >= 0, pz + rz < nz)

        def act():
            if not waiting and not own:
                name = "x"
                copy(layer, color, o, name, False).wait_recv()
            for name in sends:

                def go(name=name):
                    c = copy(layer, color, o, name, own)
                    if waiting:
                        c.wait_send()
                    else:
                        c.start()

                guarded(ends[name], go)

        guarded(valid, act)

    def own_place(layer):
        src = shard.at[pl.ds(pl.multiple_of(layer * rows, 16), rows), :]
        dst = full.at[pl.ds(pl.multiple_of((layer * n + me) * rows, 16), rows), :]
        return pltpu.make_async_copy(src, dst, own_sem.at[3 + layer])

    for phase in range(4):
        stacks = [[item for item in plan if item[0] == phase] for plan in plans]

        def step(layer, carry):
            for i in range(max(len(s) for s in stacks[:3])):
                for color in range(3):
                    if i < len(stacks[color]):
                        visit(layer, color, stacks[color][i], False)
            return carry

        lax.fori_loop(0, layers, step, 0)
        if phase == 0:
            lax.fori_loop(0, layers, lambda layer, c: (own_place(layer).start(), c)[1], 0)
            keep.wait()
            swap.wait()
        for item in stacks[3]:
            visit(0, 3, item, False)

    def finish(layer, carry):
        for color in range(3):
            for item in plans[color]:
                visit(layer, color, item, True)
        own_place(layer).wait()
        return carry

    lax.fori_loop(0, layers, finish, 0)
    for item in plans[3]:
        visit(0, 3, item, True)


def gather_rows(shards, vec, nz):
    layers, rows, cols = shards.shape
    n = 4 * nz
    any_space = pl.BlockSpec(memory_space=pl.ANY)
    vmem = pl.BlockSpec(memory_space=pltpu.VMEM)
    full, vec_full = pl.pallas_call(
        functools.partial(gather_kernel, nz, layers, rows, cols),
        out_shape=(
            jax.ShapeDtypeStruct((layers * n * rows, cols), shards.dtype),
            jax.ShapeDtypeStruct((n, 2) + vec.shape, vec.dtype),
        ),
        in_specs=[vmem, vmem],
        out_specs=(any_space, any_space),
        scratch_shapes=[
            pltpu.SemaphoreType.DMA((3 + layers,)),
            pltpu.SemaphoreType.DMA((layers, 4, n)),
            pltpu.SemaphoreType.DMA((layers, 4, 4, n)),
        ],
        compiler_params=pltpu.CompilerParams(
            collective_id=0, has_side_effects=True, vmem_limit_bytes=8 * 1024 * 1024
        ),
        name="gather_rows",
    )(shards.reshape(layers * rows, cols), vec)
    return full.reshape(layers, n * rows, cols), vec_full


def product_tiles(pairs, first, end):
    tiles = []
    at = 0
    for which, (_, right) in enumerate(pairs):
        width = right.shape[1]
        start = max(first, at)
        while start < min(end, at + width):
            size = min(512, min(end, at + width) - start)
            tiles.append((which, start - at, start, size))
            start += size
        at += width
    return tiles, at


def fill_products(pairs, vector_rows, part, first, end):
    tiles, products_end = product_tiles(pairs, first, end)
    for which, at, to, size in tiles:
        left, right = pairs[which]
        part[:, to : to + size] = lax.dot_general(
            left[...],
            right[:, at : at + size],
            (((0,), (0,)), ((), ())),
            preferred_element_type=jnp.float32,
        ).astype(part.dtype)
    if end > products_end:
        part[:, products_end:end] = vector_rows[...].T.astype(part.dtype)


def pack_kernel(*refs):
    part = refs[-1]
    pairs = [(refs[2 * i], refs[2 * i + 1]) for i in range(4)]
    fill_products(pairs, refs[8], part, 0, part.shape[1])


def pack_products(pairs, vector_rows):
    depth = pairs[0][0].shape[1]
    cols = sum(right.shape[1] for _, right in pairs) + vector_rows.shape[0]
    vmem = pl.BlockSpec(memory_space=pltpu.VMEM)
    flops = 2 * pairs[0][0].shape[0] * depth * cols
    return pl.pallas_call(
        pack_kernel,
        out_shape=jax.ShapeDtypeStruct((depth, cols), jnp.bfloat16),
        in_specs=[vmem] * 9,
        out_specs=vmem,
        compiler_params=pltpu.CompilerParams(vmem_limit_bytes=40 * 1024 * 1024),
        cost_estimate=pl.CostEstimate(
            flops=flops, bytes_accessed=2 * depth * cols, transcendentals=0
        ),
        name="pack_products",
    )(*[side for pair in pairs for side in pair], vector_rows)


def sum_kernel(nz, layers, rows, cols, *refs):
    pairs = [(refs[2 * i], refs[2 * i + 1]) for i in range(4)]
    vector_rows = refs[8]
    out, part, ra, rb, rc, ry_c, rx_c, sc, send, recv = refs[9:]
    sum_body(
        nz, layers, rows, cols, pairs, vector_rows, part, out,
        ra, rb, rc, ry_c, rx_c, sc, send, recv,
    )


def sum_body(nz, layers, rows, cols, pairs, vector_rows, part, out, ra, rb, rc, ry_c, rx_c, sc, send, recv):
    me, px, py, pz, hops = places(nz)
    tp = lax.axis_index("tp")
    n = 4 * nz
    spans = split_columns(cols)
    ends = greet(nz, pz, hops, tp, False)
    base = (0, 5 * nz, 10 * nz)
    pools = (ra, rb)
    coord = {"x": px, "y": py}
    stride = {"x": 1, "y": 2}
    zs = []
    for k in range((nz + 1) // 2):
        zs.extend([nz - 1 - k, k] if nz - 1 - k != k else [k])

    def mine(layer, o, color, count=1):
        start = pl.multiple_of((layer * n + o) * rows, 16)
        return part.at[pl.ds(start, count * rows), pl.ds(*spans[color])]

    def copy(src, dst, layer, index, name):
        return pltpu.make_async_remote_copy(
            src_ref=src,
            dst_ref=dst,
            send_sem=send.at[layer, index],
            recv_sem=recv.at[layer, index],
            device_id=(hops[name], tp),
            device_id_type=MESH,
        )

    def add(dst, sources, count=rows):
        def chunk(i, carry):
            at = pl.ds(pl.multiple_of(i * 16, 16), 16)
            total = sources[0][at, :].astype(jnp.float32)
            for s in sources[1:]:
                total = total + s[at, :].astype(jnp.float32)
            dst[at, :] = total.astype(dst.dtype)
            return carry

        lax.fori_loop(0, count // 16, chunk, 0)

    def over_layers(act):
        lax.fori_loop(0, layers, lambda layer, c: (act(layer), c)[1], 0)

    dims = (("x", "y"), ("y", "x"))

    def dest(color, flip_one, flip_two, z):
        d1, d2 = dims[color]
        c1 = coord[d1] if not flip_one else 1 - coord[d1]
        c2 = coord[d2] if not flip_two else 1 - coord[d2]
        return 4 * z + stride[d1] * c1 + stride[d2] * c2

    def hop_one(layer, color, flip_two, z):
        slot = flip_two * nz + z
        dst = pools[color].at[layer, slot]
        return copy(
            mine(layer, dest(color, 1, flip_two, z), color),
            dst,
            layer,
            base[color] + slot,
            dims[color][0],
        )

    def hop_two(layer, color, z):
        pool = pools[color]
        slot = 2 * nz + z
        return copy(
            pool.at[layer, nz + z], pool.at[layer, slot], layer, base[color] + slot, dims[color][1]
        )

    def line(layer, color, z, name):
        pool = pools[color]
        slot = (3 if name == "u" else 4) * nz + z
        return copy(
            pool.at[layer, 2 * nz + z], pool.at[layer, slot], layer, base[color] + slot, name
        )

    def line_c(layer, z, name, direct):
        slot = (0 if name == "u" else nz) + z
        dst = rc.at[layer, slot]
        src = mine(layer, 4 * z, 2, 4) if direct else dst
        return copy(src, dst, layer, base[2] + slot, name)

    def swap_y(layer):
        src = sc.at[layer, pl.ds(pl.multiple_of((1 - py) * 2 * rows, 16), 2 * rows), :]
        return copy(src, ry_c.at[layer], layer, base[2] + 2 * nz, "y")

    def swap_x(layer):
        src = ry_c.at[layer, pl.ds(pl.multiple_of((1 - px) * rows, 16), rows), :]
        return copy(src, rx_c.at[layer], layer, base[2] + 2 * nz + 1, "x")

    def start_pool(layer, color):
        for flip in (1, 0):
            for z in zs:
                hop_one(layer, color, flip, z).start()

    def start_c(layer):
        for z in zs:
            if z > 0:
                pl.when(pz == 0)(lambda z=z: line_c(layer, z, "u", True).start())
            if z < nz - 1:
                pl.when(pz == nz - 1)(lambda z=z: line_c(layer, z, "d", True).start())

    def relay_c(layer, z):
        if z > 1:

            @pl.when(jnp.logical_and(pz > 0, pz < z))
            def _():
                c = line_c(layer, z, "u", False)
                c.wait_recv()
                add(rc.at[layer, z], (mine(layer, 4 * z, 2, 4), rc.at[layer, z]), 4 * rows)
                c.start()

        if z < nz - 2:

            @pl.when(jnp.logical_and(pz < nz - 1, pz > z))
            def _():
                c = line_c(layer, z, "d", False)
                c.wait_recv()
                at = rc.at[layer, nz + z]
                add(at, (mine(layer, 4 * z, 2, 4), at), 4 * rows)
                c.start()

    def second(layer):
        for z in zs:
            for color in range(2):
                hop_one(layer, color, 1, z).wait_recv()
                at = pools[color].at[layer, nz + z]
                add(at, (mine(layer, dest(color, 0, 1, z), color), at))
                hop_two(layer, color, z).start()
            relay_c(layer, z)

    def settle_c(layer):
        up = line_c(layer, pz, "u", False)
        down = line_c(layer, pz, "d", False)
        own = mine(layer, 4 * pz, 2, 4)
        from_up = rc.at[layer, pz]
        from_down = rc.at[layer, nz + pz]
        target = sc.at[layer]

        @pl.when(pz == 0)
        def _():
            down.wait_recv()
            add(target, (own, from_down), 4 * rows)

        @pl.when(pz == nz - 1)
        def _():
            up.wait_recv()
            add(target, (own, from_up), 4 * rows)

        @pl.when(jnp.logical_and(pz > 0, pz < nz - 1))
        def _():
            down.wait_recv()
            up.wait_recv()
            add(target, (own, from_up, from_down), 4 * rows)

        swap_y(layer).start()

    def third(layer):
        for z in zs:
            for color in range(2):
                pool = pools[color]
                hop_one(layer, color, 0, z).wait_recv()
                hop_two(layer, color, z).wait_recv()
                at = pool.at[layer, 2 * nz + z]
                add(at, (mine(layer, dest(color, 0, 0, z), color), pool.at[layer, z], at))
                pl.when(jnp.logical_and(pz == 0, z > pz))(
                    lambda c=color, z=z: line(layer, c, z, "u").start()
                )
                pl.when(jnp.logical_and(pz == nz - 1, z < pz))(
                    lambda c=color, z=z: line(layer, c, z, "d").start()
                )

    def relay(layer):
        for z in zs:
            for color in range(2):
                pool = pools[color]
                at = pool.at[layer, 2 * nz + z]

                @pl.when(jnp.logical_and(pz > 0, pz < z))
                def _():
                    c = line(layer, color, z, "u")
                    c.wait_recv()
                    add(at, (at, pool.at[layer, 3 * nz + z]))
                    c.start()

                @pl.when(jnp.logical_and(pz < nz - 1, pz > z))
                def _():
                    c = line(layer, color, z, "d")
                    c.wait_recv()
                    add(at, (at, pool.at[layer, 4 * nz + z]))
                    c.start()

    def out_at(layer, color):
        return out.at[pl.ds(pl.multiple_of(layer * rows, 16), rows), pl.ds(*spans[color])]

    def x_c(layer):
        swap_y(layer).wait_recv()
        own = sc.at[layer, pl.ds(pl.multiple_of(py * 2 * rows, 16), 2 * rows), :]
        add(ry_c.at[layer], (own, ry_c.at[layer]), 2 * rows)
        swap_x(layer).start()

    def final(layer):
        for color in range(2):
            pool = pools[color]
            up = line(layer, color, pz, "u")
            down = line(layer, color, pz, "d")
            own = pool.at[layer, 2 * nz + pz]
            from_up = pool.at[layer, 3 * nz + pz]
            from_down = pool.at[layer, 4 * nz + pz]
            target = out_at(layer, color)

            @pl.when(pz == 0)
            def _():
                down.wait_recv()
                add(target, (own, from_down))

            @pl.when(pz == nz - 1)
            def _():
                up.wait_recv()
                add(target, (own, from_up))

            @pl.when(jnp.logical_and(pz > 0, pz < nz - 1))
            def _():
                down.wait_recv()
                up.wait_recv()
                add(target, (own, from_up, from_down))

        swap_x(layer).wait_recv()
        own = ry_c.at[layer, pl.ds(pl.multiple_of(px * rows, 16), rows), :]
        add(out_at(layer, 2), (own, rx_c.at[layer]))

    def drain(layer):
        for z in zs:
            for color in range(2):
                hop_one(layer, color, 1, z).wait_send()
                hop_one(layer, color, 0, z).wait_send()
                hop_two(layer, color, z).wait_send()
                pl.when(pz < z)(lambda c=color, z=z: line(layer, c, z, "u").wait_send())
                pl.when(pz > z)(lambda c=color, z=z: line(layer, c, z, "d").wait_send())
            pl.when(pz < z)(lambda z=z: line_c(layer, z, "u", False).wait_send())
            pl.when(pz > z)(lambda z=z: line_c(layer, z, "d", False).wait_send())
        swap_y(layer).wait_send()
        swap_x(layer).wait_send()

    def fill(color):
        first, width = spans[color]
        fill_products(pairs, vector_rows, part, first, first + width)

    fill(0)
    fill(1)
    start_pool(0, 0)
    fill(2)
    start_pool(0, 1)
    start_c(0)
    for act in (second, settle_c, third, x_c, relay, final, drain):
        over_layers(act)


def sum_rows(pairs, vector_rows, nz):
    layers = 1
    depth = pairs[0][0].shape[1]
    cols = sum(right.shape[1] for _, right in pairs) + vector_rows.shape[0]
    n = 4 * nz
    rows = depth // n
    spans = split_columns(cols)
    vmem = pl.BlockSpec(memory_space=pltpu.VMEM)
    dt = jnp.bfloat16
    count = 12 * nz + 2
    out = pl.pallas_call(
        functools.partial(sum_kernel, nz, layers, rows, cols),
        out_shape=jax.ShapeDtypeStruct((layers * rows, cols), jnp.float32),
        in_specs=[vmem] * 9,
        out_specs=vmem,
        scratch_shapes=[
            pltpu.VMEM((depth, cols), dt),
            pltpu.VMEM((layers, 5 * nz, rows, spans[0][1]), dt),
            pltpu.VMEM((layers, 5 * nz, rows, spans[1][1]), dt),
            pltpu.VMEM((layers, 2 * nz, 4 * rows, spans[2][1]), dt),
            pltpu.VMEM((layers, 2 * rows, spans[2][1]), dt),
            pltpu.VMEM((layers, rows, spans[2][1]), dt),
            pltpu.VMEM((layers, 4 * rows, spans[2][1]), dt),
            pltpu.SemaphoreType.DMA((layers, count)),
            pltpu.SemaphoreType.DMA((layers, count)),
        ],
        compiler_params=pltpu.CompilerParams(
            collective_id=1, has_side_effects=True, vmem_limit_bytes=60 * 1024 * 1024
        ),
        name="sum_rows",
    )(*[side for pair in pairs for side in pair], vector_rows)
    return out


def scaled_scores(q, k, same):
    scores = mul(q, k, ((1,), (1,))) * SCORE_SCALE
    return jnp.where(same, scores, MASK_FILL)


def attention_kernel(chunk, joined, seg_col, seg_row, context, log_total):
    length, cols = context.shape
    for start in range(0, length, chunk):
        at = pl.ds(start, chunk)
        same = seg_col[at, :] == seg_row[...]
        lane = lax.broadcasted_iota(jnp.int32, (chunk, LANES), 1)
        logs = jnp.zeros((chunk, LANES), jnp.float32)
        for first in range(0, cols, LANES):
            q_pair = joined[at, first : first + LANES]
            k_pair = joined[:, cols + first : cols + first + LANES]
            v_pair = joined[:, 2 * cols + first : 2 * cols + first + LANES]
            made = []
            for low in range(0, LANES, HEAD_DIM):
                part = slice(low, low + HEAD_DIM)
                scores = scaled_scores(q_pair[:, part], k_pair[:, part], same)
                top = jnp.max(scores, axis=1, keepdims=True)
                exponent = jnp.exp(scores - top)
                total = jnp.sum(exponent, axis=1, keepdims=True)
                probs = (exponent / total).astype(jnp.bfloat16)
                made.append(mul(probs, v_pair[:, part], ((1,), (0,))))
                head = (first + low) // HEAD_DIM
                logs = jnp.where(lane == head, top + jnp.log(total), logs)
            context[at, first : first + LANES] = jnp.concatenate(made, axis=1).astype(
                jnp.bfloat16
            )
        log_total[at, :] = logs


def attention_back_kernel(
    chunk, joined, context_low, log_total, seg_col, seg_row, joined_grad, column_sums
):
    length, cols = context_low.shape
    for first in range(0, cols, LANES):
        k_pair = joined[:, cols + first : cols + first + LANES]
        v_pair = joined[:, 2 * cols + first : 2 * cols + first + LANES]
        key_sums = [None] * (LANES // HEAD_DIM)
        value_sums = [None] * (LANES // HEAD_DIM)
        query_column = jnp.zeros((1, LANES), jnp.float32)
        for start in range(0, length, chunk):
            at = pl.ds(start, chunk)
            same = seg_col[at, :] == seg_row[...]
            q_pair = joined[at, first : first + LANES]
            c_pair = context_low[at, first : first + LANES]
            logs = log_total[at, :]
            made = []
            for which, low in enumerate(range(0, LANES, HEAD_DIM)):
                part = slice(low, low + HEAD_DIM)
                q, k, v, c = q_pair[:, part], k_pair[:, part], v_pair[:, part], c_pair[:, part]
                head = (first + low) // HEAD_DIM
                probabilities = jnp.exp(scaled_scores(q, k, same) - logs[:, head : head + 1])
                prob_grad = mul(c, v, ((1,), (1,)))
                row_delta = jnp.sum(prob_grad * probabilities, axis=1, keepdims=True)
                score_grad = (probabilities * (prob_grad - row_delta)).astype(jnp.bfloat16)
                value_part = mul(probabilities.astype(jnp.bfloat16), c, ((0,), (0,)))
                key_part = mul(score_grad, q, ((0,), (0,)))
                made.append(mul(score_grad, k, ((1,), (0,))))
                if start:
                    value_part = value_part + value_sums[which]
                    key_part = key_part + key_sums[which]
                value_sums[which] = value_part
                key_sums[which] = key_part
            query_grad = (jnp.concatenate(made, axis=1) * SCORE_SCALE).astype(jnp.bfloat16)
            joined_grad[at, first : first + LANES] = query_grad
            query_column = query_column + jnp.sum(
                query_grad.astype(jnp.float32), axis=0, keepdims=True
            )
        key_grad = (jnp.concatenate(key_sums, axis=1) * SCORE_SCALE).astype(jnp.bfloat16)
        value_grad = jnp.concatenate(value_sums, axis=1).astype(jnp.bfloat16)
        joined_grad[:, cols + first : cols + first + LANES] = key_grad
        joined_grad[:, 2 * cols + first : 2 * cols + first + LANES] = value_grad
        column_sums[0:1, first : first + LANES] = query_column
        column_sums[1:2, first : first + LANES] = jnp.sum(
            value_grad.astype(jnp.float32), axis=0, keepdims=True
        )


def local_kernel(body, shapes, work, name, *arrays):
    vmem = pl.BlockSpec(memory_space=pltpu.VMEM)
    return pl.pallas_call(
        body,
        out_shape=shapes,
        in_specs=[vmem] * len(arrays),
        out_specs=tuple(vmem for _ in shapes),
        compiler_params=pltpu.CompilerParams(vmem_limit_bytes=40 * 1024 * 1024),
        cost_estimate=pl.CostEstimate(flops=work, bytes_accessed=1 << 22, transcendentals=1 << 21),
        name=name,
    )(*arrays)


def pair_sum(rows, tp_rank):
    layers, depth, cols = rows.shape
    halves = rows.reshape(layers, 2, depth // 2, cols)
    away = lax.dynamic_index_in_dim(halves, 1 - tp_rank, 1, keepdims=False)
    mine = lax.dynamic_index_in_dim(halves, tp_rank, 1, keepdims=False)
    return mine + lax.ppermute(away, "tp", [(0, 1), (1, 0)])


def per_device(
    block_input,
    cotangent,
    qkv_weight,
    proj_weight,
    fc1_weight,
    fc2_weight,
    norm_gains,
    biases,
    fc1_bias,
    segments,
    keep_flags,
):
    local_len, row_count, width = block_input.shape
    assert row_count == 1
    tp_rank = lax.axis_index("tp")
    tp_size = lax.axis_size("tp")
    full_len = local_len * tp_size
    shard_rows = qkv_weight.shape[1]
    head_cols = qkv_weight.shape[3]
    ff_cols = fc1_weight.shape[2]
    qkv_end = 3 * head_cols
    proj_end = qkv_end + head_cols
    fc1_end = proj_end + ff_cols
    bf16 = jnp.bfloat16
    f32 = jnp.float32

    segment_row = segments[0]
    local_segments = lax.dynamic_slice_in_dim(segment_row, tp_rank * local_len, local_len, 0)
    member = (
        local_segments[:, None] == jnp.arange(SEGS, dtype=jnp.int32)[None, :]
    ).astype(f32)

    def token_keep(keep_row):
        return jnp.sum(member * keep_row.astype(f32), axis=1, keepdims=True)

    def place(part_grad, total_len):
        return lax.dynamic_update_slice_in_dim(
            jnp.zeros((total_len,), f32), part_grad, tp_rank * part_grad.shape[0], 0
        )

    def gather_positions(local_rows):
        return lax.all_gather(local_rows, "tp", axis=0, tiled=True)

    def scatter_positions(partial):
        if tp_size == 2:
            halves = partial.reshape(2, local_len, width)
            away = lax.dynamic_index_in_dim(halves, 1 - tp_rank, 0, keepdims=False)
            mine = lax.dynamic_index_in_dim(halves, tp_rank, 0, keepdims=False)
            arrived = lax.ppermute(away, "tp", [(0, 1), (1, 0)])
            return mine.astype(f32) + arrived.astype(f32)
        return lax.psum_scatter(partial, "tp", scatter_dimension=0, tiled=True).astype(f32)

    row_devices = lax.axis_size("rows")
    own_kernels = shard_rows % 16 == 0 and row_devices % 4 == 0 and tp_size == 2
    shards = (
        [
            jnp.concatenate(
                [
                    qkv_weight[layer].reshape(shard_rows, qkv_end).astype(bf16),
                    proj_weight[layer].T.astype(bf16),
                    fc1_weight[layer].astype(bf16),
                    fc2_weight[layer].T.astype(bf16),
                ],
                axis=1,
            )
            for layer in range(LAYERS)
        ]
    )
    vector_parts = [norm_gains, biases, fc1_bias[:, None, :]]
    vector_flat = jnp.concatenate([part.reshape(-1) for part in vector_parts])
    if own_kernels:
        filled = -(-vector_flat.size // (8 * LANES)) * 8 * LANES
        packed_first, vector_full = gather_rows(
            shards[0][None],
            jnp.pad(vector_flat, (0, filled - vector_flat.size)).reshape(-1, LANES),
            row_devices // 4,
        )
        vector_full = vector_full.reshape(row_devices * tp_size, -1)
        packed_full = [packed_first[0]] + [
            lax.all_gather(shard, "rows", axis=0, tiled=True) for shard in shards[1:]
        ]
    else:
        packed_full = [lax.all_gather(shard, "rows", axis=0, tiled=True) for shard in shards]
        vector_full = lax.all_gather(vector_flat, ("rows", "tp"), axis=0, tiled=False)
    full_vectors = []
    first = 0
    for part in vector_parts:
        taken = vector_full[:, first : first + part.size].reshape((-1,) + part.shape)
        first += part.size
        full_vectors.append(jnp.moveaxis(taken, 0, 2).reshape(part.shape[0], part.shape[1], -1))
    gains_full, biases_full, fc1_bias_full = full_vectors

    stream = block_input[:, 0]
    saved = []
    for layer in range(LAYERS):
        packed = packed_full[layer]
        w_qkv = packed[:, :qkv_end]
        w_proj = packed[:, qkv_end:proj_end]
        w_fc1 = packed[:, proj_end:fc1_end]
        w_fc2 = packed[:, fc1_end:]
        gain = gains_full[layer]
        bias = biases_full[layer]
        in_bias = jnp.concatenate(
            [
                lax.dynamic_slice_in_dim(bias[1], tp_rank * head_cols, head_cols, 0),
                jnp.zeros((head_cols,), f32),
                lax.dynamic_slice_in_dim(bias[2], tp_rank * head_cols, head_cols, 0),
            ]
        )
        up_bias = lax.dynamic_slice_in_dim(fc1_bias_full[layer, 0], tp_rank * ff_cols, ff_cols, 0)
        keep_attn = token_keep(keep_flags[layer, 0])
        keep_mlp = token_keep(keep_flags[layer, 1])
        xhat_one, rstd_one = apply_layer_norm(stream)
        normed_one = gather_positions((xhat_one * gain[0] + bias[0]).astype(bf16))
        joined = (mul(normed_one, w_qkv, ((1,), (0,))) + in_bias).astype(bf16)
        context, log_total = local_kernel(
            functools.partial(attention_kernel, full_len // 2),
            (
                jax.ShapeDtypeStruct((full_len, head_cols), bf16),
                jax.ShapeDtypeStruct((full_len, LANES), f32),
            ),
            4 * full_len * full_len * head_cols,
            "attention",
            joined,
            segment_row[:, None],
            segment_row[None],
        )
        attn = scatter_positions(mul(context, w_proj, ((1,), (1,))).astype(bf16)) + bias[3]
        middle = stream + keep_attn * attn / KEEP_RATE
        xhat_two, rstd_two = apply_layer_norm(middle)
        normed_two = gather_positions((xhat_two * gain[1] + bias[4]).astype(bf16))
        hidden_pre = mul(normed_two, w_fc1, ((1,), (0,))) + up_bias
        hidden = (hidden_pre * cumulative(hidden_pre)).astype(bf16)
        mlp = scatter_positions(mul(hidden, w_fc2, ((1,), (1,))).astype(bf16)) + bias[5]
        stream = middle + keep_mlp * mlp / KEEP_RATE
        saved.append(
            (
                (w_qkv, w_proj, w_fc1, w_fc2, gain, keep_attn, keep_mlp),
                (xhat_one, rstd_one, normed_one, joined, log_total, context),
                (xhat_two, rstd_two, normed_two, hidden_pre, hidden),
            )
        )

    grad = cotangent[:, 0]
    weight_grads = [None] * LAYERS
    for layer in reversed(range(LAYERS)):
        (w_qkv, w_proj, w_fc1, w_fc2, gain, keep_attn, keep_mlp), attn_side, mlp_side = saved[layer]
        xhat_one, rstd_one, normed_one, joined, log_total, context = attn_side
        xhat_two, rstd_two, normed_two, hidden_pre, hidden = mlp_side
        mlp_grad = grad * keep_mlp / KEEP_RATE
        fc2_bias_grad = jnp.sum(mlp_grad, axis=0)
        mlp_low = gather_positions(mlp_grad.astype(bf16))
        hidden_grad = mul(mlp_low, w_fc2, ((1,), (0,)))
        pre_grad = (hidden_grad * gelu_slope(hidden_pre)).astype(bf16)
        fc1_bias_grad = jnp.sum(pre_grad.astype(f32), axis=0)
        two_grad = scatter_positions(mul(pre_grad, w_fc1, ((1,), (1,))).astype(bf16))
        gain_two_grad = jnp.sum(two_grad * xhat_two, axis=0)
        shift_two_grad = jnp.sum(two_grad, axis=0)
        middle_grad = grad + norm_backward(two_grad, xhat_two, rstd_two, gain[1])
        attn_grad = middle_grad * keep_attn / KEEP_RATE
        proj_bias_grad = jnp.sum(attn_grad, axis=0)
        attn_low = gather_positions(attn_grad.astype(bf16))
        context_low = mul(attn_low, w_proj, ((1,), (0,))).astype(bf16)
        joined_grad, in_bias_grad = local_kernel(
            functools.partial(attention_back_kernel, full_len // 2),
            (
                jax.ShapeDtypeStruct((full_len, 3 * head_cols), bf16),
                jax.ShapeDtypeStruct((2, head_cols), f32),
            ),
            10 * full_len * full_len * head_cols,
            "attention_back",
            joined,
            context_low,
            log_total,
            segment_row[:, None],
            segment_row[None],
        )
        one_grad = scatter_positions(mul(joined_grad, w_qkv, ((1,), (1,))).astype(bf16))
        gain_one_grad = jnp.sum(one_grad * xhat_one, axis=0)
        shift_one_grad = jnp.sum(one_grad, axis=0)
        grad = middle_grad + norm_backward(one_grad, xhat_one, rstd_one, gain[0])
        vector_rows = jnp.concatenate(
            [
                gain_one_grad[None],
                gain_two_grad[None],
                shift_one_grad[None],
                place(in_bias_grad[0], width)[None],
                place(in_bias_grad[1], width)[None],
                proj_bias_grad[None],
                shift_two_grad[None],
                fc2_bias_grad[None],
                place(fc1_bias_grad, ff_cols * tp_size).reshape(width, -1).T,
            ],
            axis=0,
        )
        vector_rows = jnp.pad(vector_rows, ((0, LANES - vector_rows.shape[0]), (0, 0)))
        pairs = [
            (normed_one, joined_grad),
            (attn_low, context),
            (normed_two, pre_grad),
            (mlp_low, hidden),
        ]
        if own_kernels and layer in KERNEL_LAYERS:
            weight_grads[layer] = sum_rows(pairs, vector_rows, row_devices // 4)
        else:
            packed = pack_products(pairs, vector_rows)
            if layer:
                packed, grad = lax.optimization_barrier((packed, grad))
            weight_grads[layer] = lax.psum_scatter(
                packed, "rows", scatter_dimension=0, tiled=True
            ).astype(f32)

    weight_sum = jnp.stack(weight_grads)
    fc2_end = fc1_end + ff_cols
    vector_sum = lax.psum_scatter(
        weight_sum[:, :, fc2_end:], "tp", scatter_dimension=1, tiled=True
    ) if tp_size != 2 else pair_sum(weight_sum[:, :, fc2_end:], tp_rank)
    vector_rows = jnp.transpose(vector_sum[:, :, :8], (0, 2, 1))
    return (
        stream[:, None],
        grad[:, None],
        weight_sum[:, :, :qkv_end].reshape(LAYERS, shard_rows, 3, head_cols),
        jnp.transpose(weight_sum[:, :, qkv_end:proj_end], (0, 2, 1)),
        weight_sum[:, :, proj_end:fc1_end],
        jnp.transpose(weight_sum[:, :, fc1_end:fc2_end], (0, 2, 1)),
        vector_rows[:, :2],
        vector_rows[:, 2:8],
        vector_sum[:, :, 8 : 8 + ff_cols * tp_size // width].reshape(LAYERS, -1),
    )


def solution(mesh):
    placed = (
        P("tp", "rows", None),
        P("tp", "rows", None),
        P(None, "rows", None, "tp"),
        P(None, "tp", "rows"),
        P(None, "rows", "tp"),
        P(None, "tp", "rows"),
        P(None, None, ("rows", "tp")),
        P(None, None, ("rows", "tp")),
        P(None, ("rows", "tp")),
        P("rows", None),
        P(None, None, "rows", None),
    )
    return jax.shard_map(
        per_device,
        mesh=mesh,
        in_specs=placed,
        out_specs=placed[:2] + placed[2:9],
        check_vma=False,
    )
```

```python
import functools
import math

import jax
import jax.numpy as jnp
from jax import lax
from jax.experimental import pallas as pl
from jax.experimental.pallas import tpu as pltpu
from jax.sharding import PartitionSpec as P


MESH = pl.DeviceIdType.MESH
LANES = 128
GATHER_ORDERS = ("zyx", "zxy", "xyz")
HEAD_DIM = 64
LAYERS = 2
SEGS = 8

NORM_EPS = 1e-06
KEEP_RATE = 0.9
SCORE_SCALE = 0.125
MASK_FILL = -1e30
INV_SQRT_TWO = 1.0 / math.sqrt(2.0)
INV_SQRT_TWO_PI = 1.0 / math.sqrt(2.0 * math.pi)


def apply_layer_norm(residual_rows):
    center = residual_rows - jnp.mean(residual_rows, axis=-1, keepdims=True)
    spread = jnp.mean(center * center, axis=-1, keepdims=True)
    inverse_deviation = lax.rsqrt(spread + NORM_EPS)
    return (center * inverse_deviation, inverse_deviation)


def norm_backward(normed_gradient, centered_unit, inverse_deviation, norm_gain):
    scaled_rows = normed_gradient * norm_gain
    return inverse_deviation * (
        scaled_rows
        - jnp.mean(scaled_rows, axis=-1, keepdims=True)
        - centered_unit * jnp.mean(scaled_rows * centered_unit, axis=-1, keepdims=True)
    )


def cumulative(u):
    return 0.5 * (1.0 + lax.erf(u * INV_SQRT_TWO))


def gelu_slope(u):
    return cumulative(u) + u * jnp.exp(-0.5 * u * u) * INV_SQRT_TWO_PI


def mul(a, b, dims):
    return lax.dot_general(a, b, (dims, ((), ())), preferred_element_type=jnp.float32)


def split_columns(total):
    groups = total // LANES
    first = groups * 14 // 36
    return (
        (0, first * LANES),
        (first * LANES, first * LANES),
        (2 * first * LANES, (groups - 2 * first) * LANES),
    )


def places(nz):
    me = lax.axis_index("rows")
    px = lax.rem(me, 2)
    py = lax.rem(lax.div(me, 2), 2)
    pz = lax.div(me, 4)
    hops = {
        "x": me + 1 - 2 * px,
        "y": me + 2 - 4 * py,
        "u": lax.min(me + 4, 4 * nz - 1),
        "d": lax.max(me - 4, 0),
    }
    return me, px, py, pz, hops


def guarded(cond, act):
    if cond is None:
        act()
    else:
        pl.when(cond)(act)


def both(a, b):
    if a is None:
        return b
    if b is None:
        return a
    return jnp.logical_and(a, b)


def greet(nz, pz, hops, tp, with_tp):
    barrier = pltpu.get_barrier_semaphore()
    ends = {"x": None, "y": None, "u": pz < nz - 1, "d": pz > 0}
    for name, cond in ends.items():
        guarded(
            cond,
            lambda name=name: pl.semaphore_signal(
                barrier, inc=1, device_id=(hops[name], tp), device_id_type=MESH
            ),
        )
    waits = 2
    if with_tp:
        pl.semaphore_signal(
            barrier, inc=1, device_id=(lax.axis_index("rows"), 1 - tp), device_id_type=MESH
        )
        waits = 3
    waits = waits + lax.min(pz, 1) + lax.min(nz - 1 - pz, 1)
    pl.semaphore_wait(barrier, waits)
    return ends


def gather_plan(order, nz):
    found = []
    for rx in (0, 1):
        for ry in (0, 1):
            for rz in range(1 - nz, nz):
                rel = {"x": rx, "y": ry, "z": rz}
                differing = [i for i, dim in enumerate(order) if rel[dim]]
                last = differing[-1] if differing else -1
                sends = []
                if last >= 0 and order[last] == "z":
                    sends.append("u" if rz < 0 else "d")
                for dim in order[last + 1 :]:
                    sends.extend("ud" if dim == "z" else dim)
                found.append((last + 1, abs(rz), rx + ry, rx, ry, rz, tuple(sends)))
    return sorted(found)


def gather_kernel(nz, layers, rows, cols, shard, vec, full, vec_full, own_sem, recv, send):
    me, px, py, pz, hops = places(nz)
    tp = lax.axis_index("tp")
    n = 4 * nz
    spans = split_columns(cols)
    names = "xyud"
    ends = greet(nz, pz, hops, tp, True)

    def origin(rx, ry, rz):
        return me + rx * (1 - 2 * px) + ry * 2 * (1 - 2 * py) + 4 * rz

    def block(layer, color, o):
        start = pl.multiple_of((layer * n + o) * rows, 16)
        return full.at[pl.ds(start, rows), pl.ds(*spans[color])]

    def copy(layer, color, o, name, own):
        if color == 3:
            src = vec_full.at[o]
            dst = vec_full.at[o]
        else:
            dst = block(layer, color, o)
            src = dst
            if own:
                start = pl.multiple_of(layer * rows, 16)
                src = shard.at[pl.ds(start, rows), pl.ds(*spans[color])]
        return pltpu.make_async_remote_copy(
            src_ref=src,
            dst_ref=dst,
            send_sem=send.at[layer, color, names.index(name), o],
            recv_sem=recv.at[layer, color, o],
            device_id=(hops[name], tp),
            device_id_type=MESH,
        )

    keep = pltpu.make_async_copy(vec, vec_full.at[me, tp], own_sem.at[0])
    keep.start()
    swap = pltpu.make_async_remote_copy(
        src_ref=vec,
        dst_ref=vec_full.at[me, tp],
        send_sem=own_sem.at[1],
        recv_sem=own_sem.at[2],
        device_id=(me, 1 - tp),
        device_id_type=MESH,
    )
    swap.start()
    plans = [gather_plan(order, nz) for order in GATHER_ORDERS + ("xyz",)]

    def visit(layer, color, item, waiting):
        _, _, _, rx, ry, rz, sends = item
        o = origin(rx, ry, rz)
        own = (rx, ry, rz) == (0, 0, 0)
        valid = None if rz == 0 else jnp.logical_and(pz + rz >= 0, pz + rz < nz)

        def act():
            if not waiting and not own:
                name = "x"
                copy(layer, color, o, name, False).wait_recv()
            for name in sends:

                def go(name=name):
                    c = copy(layer, color, o, name, own)
                    if waiting:
                        c.wait_send()
                    else:
                        c.start()

                guarded(ends[name], go)

        guarded(valid, act)

    def own_place(layer):
        src = shard.at[pl.ds(pl.multiple_of(layer * rows, 16), rows), :]
        dst = full.at[pl.ds(pl.multiple_of((layer * n + me) * rows, 16), rows), :]
        return pltpu.make_async_copy(src, dst, own_sem.at[3 + layer])

    for phase in range(4):
        stacks = [[item for item in plan if item[0] == phase] for plan in plans]

        def step(layer, carry):
            for i in range(max(len(s) for s in stacks[:3])):
                for color in range(3):
                    if i < len(stacks[color]):
                        visit(layer, color, stacks[color][i], False)
            return carry

        lax.fori_loop(0, layers, step, 0)
        if phase == 0:
            lax.fori_loop(0, layers, lambda layer, c: (own_place(layer).start(), c)[1], 0)
            keep.wait()
            swap.wait()
        for item in stacks[3]:
            visit(0, 3, item, False)

    def finish(layer, carry):
        for color in range(3):
            for item in plans[color]:
                visit(layer, color, item, True)
        own_place(layer).wait()
        return carry

    lax.fori_loop(0, layers, finish, 0)
    for item in plans[3]:
        visit(0, 3, item, True)


def gather_rows(shards, vec, nz):
    layers, rows, cols = shards.shape
    n = 4 * nz
    any_space = pl.BlockSpec(memory_space=pl.ANY)
    vmem = pl.BlockSpec(memory_space=pltpu.VMEM)
    full, vec_full = pl.pallas_call(
        functools.partial(gather_kernel, nz, layers, rows, cols),
        out_shape=(
            jax.ShapeDtypeStruct((layers * n * rows, cols), shards.dtype),
            jax.ShapeDtypeStruct((n, 2) + vec.shape, vec.dtype),
        ),
        in_specs=[vmem, vmem],
        out_specs=(any_space, any_space),
        scratch_shapes=[
            pltpu.SemaphoreType.DMA((3 + layers,)),
            pltpu.SemaphoreType.DMA((layers, 4, n)),
            pltpu.SemaphoreType.DMA((layers, 4, 4, n)),
        ],
        compiler_params=pltpu.CompilerParams(
            collective_id=0, has_side_effects=True, vmem_limit_bytes=8 * 1024 * 1024
        ),
        name="gather_rows",
    )(shards.reshape(layers * rows, cols), vec)
    return full.reshape(layers, n * rows, cols), vec_full


def product_tiles(pairs, first, end):
    tiles = []
    at = 0
    for which, (_, right) in enumerate(pairs):
        width = right.shape[1]
        start = max(first, at)
        while start < min(end, at + width):
            size = min(512, min(end, at + width) - start)
            tiles.append((which, start - at, start, size))
            start += size
        at += width
    return tiles, at


def fill_products(pairs, vector_rows, part, first, end):
    tiles, products_end = product_tiles(pairs, first, end)
    for which, at, to, size in tiles:
        left, right = pairs[which]
        part[:, to : to + size] = lax.dot_general(
            left[...],
            right[:, at : at + size],
            (((0,), (0,)), ((), ())),
            preferred_element_type=jnp.float32,
        ).astype(part.dtype)
    if end > products_end:
        part[:, products_end:end] = vector_rows[...].T.astype(part.dtype)


def pack_kernel(count, *refs):
    part = refs[-1]
    pairs = [(refs[2 * i], refs[2 * i + 1]) for i in range(count)]
    fill_products(pairs, refs[2 * count], part, 0, part.shape[1])


def pack_products(pairs, vector_rows=None):
    depth = pairs[0][0].shape[1]
    cols = sum(right.shape[1] for _, right in pairs)
    operands = [side for pair in pairs for side in pair]
    if vector_rows is not None:
        cols += vector_rows.shape[0]
        operands.append(vector_rows)
    vmem = pl.BlockSpec(memory_space=pltpu.VMEM)
    flops = 2 * pairs[0][0].shape[0] * depth * cols
    return pl.pallas_call(
        functools.partial(pack_kernel, len(pairs)),
        out_shape=jax.ShapeDtypeStruct((depth, cols), jnp.bfloat16),
        in_specs=[vmem] * len(operands),
        out_specs=vmem,
        compiler_params=pltpu.CompilerParams(vmem_limit_bytes=40 * 1024 * 1024),
        cost_estimate=pl.CostEstimate(
            flops=flops, bytes_accessed=2 * depth * cols, transcendentals=0
        ),
        name="pack_products",
    )(*operands)


def sum_kernel(nz, count, rows, cols, *refs):
    pairs = [(refs[2 * i], refs[2 * i + 1]) for i in range(count)]
    vector_rows = refs[2 * count]
    outs = refs[2 * count + 1 : 2 * count + 6]
    part, ra, rb, rc, ry_c, rx_c, sc, send, recv, out = refs[2 * count + 6 :]
    sum_body(
        nz, 1, rows, cols, pairs, vector_rows, part, out,
        ra, rb, rc, ry_c, rx_c, sc, send, recv,
    )
    qkv_out, proj_out, fc1_out, fc2_out, vector_out = outs
    at = 0
    for layer in reversed(range(LAYERS)):
        for kind in range(3):
            wide = qkv_out.shape[3]
            qkv_out[layer, :, kind, :] = out[:, at : at + wide]
            at += wide
        wide = proj_out.shape[1]
        proj_out[layer] = out[:, at : at + wide].T
        at += wide
    wide = fc1_out.shape[1]
    fc1_out[...] = out[:, at : at + wide]
    fc2_out[...] = out[:, at + wide : at + 2 * wide].T
    vector_out[...] = out[:, at + 2 * wide :]


def sum_body(nz, layers, rows, cols, pairs, vector_rows, part, out, ra, rb, rc, ry_c, rx_c, sc, send, recv):
    me, px, py, pz, hops = places(nz)
    tp = lax.axis_index("tp")
    n = 4 * nz
    spans = split_columns(cols)
    ends = greet(nz, pz, hops, tp, False)
    base = (0, 5 * nz, 10 * nz)
    pools = (ra, rb)
    coord = {"x": px, "y": py}
    stride = {"x": 1, "y": 2}
    zs = []
    for k in range((nz + 1) // 2):
        zs.extend([nz - 1 - k, k] if nz - 1 - k != k else [k])

    def mine(layer, o, color, count=1):
        start = pl.multiple_of((layer * n + o) * rows, 16)
        return part.at[pl.ds(start, count * rows), pl.ds(*spans[color])]

    def copy(src, dst, layer, index, name):
        return pltpu.make_async_remote_copy(
            src_ref=src,
            dst_ref=dst,
            send_sem=send.at[layer, index],
            recv_sem=recv.at[layer, index],
            device_id=(hops[name], tp),
            device_id_type=MESH,
        )

    def add(dst, sources, count=rows):
        def chunk(i, carry):
            at = pl.ds(pl.multiple_of(i * 16, 16), 16)
            total = sources[0][at, :].astype(jnp.float32)
            for s in sources[1:]:
                total = total + s[at, :].astype(jnp.float32)
            dst[at, :] = total.astype(dst.dtype)
            return carry

        lax.fori_loop(0, count // 16, chunk, 0)

    dims = (("x", "y"), ("y", "x"))

    def dest(color, flip_one, flip_two, z):
        d1, d2 = dims[color]
        c1 = coord[d1] if not flip_one else 1 - coord[d1]
        c2 = coord[d2] if not flip_two else 1 - coord[d2]
        return 4 * z + stride[d1] * c1 + stride[d2] * c2

    def hop_one(layer, color, flip_two, z):
        slot = flip_two * nz + z
        dst = pools[color].at[layer, slot]
        return copy(
            mine(layer, dest(color, 1, flip_two, z), color),
            dst,
            layer,
            base[color] + slot,
            dims[color][0],
        )

    def hop_two(layer, color, z):
        pool = pools[color]
        slot = 2 * nz + z
        return copy(
            pool.at[layer, nz + z], pool.at[layer, slot], layer, base[color] + slot, dims[color][1]
        )

    def line(layer, color, z, name):
        pool = pools[color]
        slot = (3 if name == "u" else 4) * nz + z
        return copy(
            pool.at[layer, 2 * nz + z], pool.at[layer, slot], layer, base[color] + slot, name
        )

    def line_c(layer, z, name, direct):
        slot = (0 if name == "u" else nz) + z
        dst = rc.at[layer, slot]
        src = mine(layer, 4 * z, 2, 4) if direct else dst
        return copy(src, dst, layer, base[2] + slot, name)

    def swap_y(layer):
        src = sc.at[layer, pl.ds(pl.multiple_of((1 - py) * 2 * rows, 16), 2 * rows), :]
        return copy(src, ry_c.at[layer], layer, base[2] + 2 * nz, "y")

    def swap_x(layer):
        src = ry_c.at[layer, pl.ds(pl.multiple_of((1 - px) * rows, 16), rows), :]
        return copy(src, rx_c.at[layer], layer, base[2] + 2 * nz + 1, "x")

    def issue(z):
        for flip in (1, 0):
            for color in range(2):
                hop_one(0, color, flip, z).start()

    def start_c(layer):
        for z in zs:
            if z > 0:
                pl.when(pz == 0)(lambda z=z: line_c(layer, z, "u", True).start())
            if z < nz - 1:
                pl.when(pz == nz - 1)(lambda z=z: line_c(layer, z, "d", True).start())

    def relay_c(layer, z):
        if z > 1:

            @pl.when(jnp.logical_and(pz > 0, pz < z))
            def _():
                c = line_c(layer, z, "u", False)
                c.wait_recv()
                add(rc.at[layer, z], (mine(layer, 4 * z, 2, 4), rc.at[layer, z]), 4 * rows)
                c.start()

        if z < nz - 2:

            @pl.when(jnp.logical_and(pz < nz - 1, pz > z))
            def _():
                c = line_c(layer, z, "d", False)
                c.wait_recv()
                at = rc.at[layer, nz + z]
                add(at, (mine(layer, 4 * z, 2, 4), at), 4 * rows)
                c.start()

    def second(layer, z):
        for color in range(2):
            hop_one(layer, color, 1, z).wait_recv()
            at = pools[color].at[layer, nz + z]
            add(at, (mine(layer, dest(color, 0, 1, z), color), at))
            hop_two(layer, color, z).start()

    def settle_c(layer):
        up = line_c(layer, pz, "u", False)
        down = line_c(layer, pz, "d", False)
        own = mine(layer, 4 * pz, 2, 4)
        from_up = rc.at[layer, pz]
        from_down = rc.at[layer, nz + pz]
        target = sc.at[layer]

        @pl.when(pz == 0)
        def _():
            down.wait_recv()
            add(target, (own, from_down), 4 * rows)

        @pl.when(pz == nz - 1)
        def _():
            up.wait_recv()
            add(target, (own, from_up), 4 * rows)

        @pl.when(jnp.logical_and(pz > 0, pz < nz - 1))
        def _():
            down.wait_recv()
            up.wait_recv()
            add(target, (own, from_up, from_down), 4 * rows)

        swap_y(layer).start()

    def third(layer, z):
        for color in range(2):
            pool = pools[color]
            hop_one(layer, color, 0, z).wait_recv()
            hop_two(layer, color, z).wait_recv()
            at = pool.at[layer, 2 * nz + z]
            add(at, (mine(layer, dest(color, 0, 0, z), color), pool.at[layer, z], at))
            pl.when(jnp.logical_and(pz == 0, z > pz))(
                lambda color=color: line(layer, color, z, "u").start()
            )
            pl.when(jnp.logical_and(pz == nz - 1, z < pz))(
                lambda color=color: line(layer, color, z, "d").start()
            )

    def relay(layer, z):
        for color in range(2):
            pool = pools[color]
            at = pool.at[layer, 2 * nz + z]

            @pl.when(jnp.logical_and(pz > 0, pz < z))
            def _():
                c = line(layer, color, z, "u")
                c.wait_recv()
                add(at, (at, pool.at[layer, 3 * nz + z]))
                c.start()

            @pl.when(jnp.logical_and(pz < nz - 1, pz > z))
            def _():
                c = line(layer, color, z, "d")
                c.wait_recv()
                add(at, (at, pool.at[layer, 4 * nz + z]))
                c.start()

    def out_at(layer, color):
        return out.at[pl.ds(pl.multiple_of(layer * rows, 16), rows), pl.ds(*spans[color])]

    def x_c(layer):
        swap_y(layer).wait_recv()
        own = sc.at[layer, pl.ds(pl.multiple_of(py * 2 * rows, 16), 2 * rows), :]
        add(ry_c.at[layer], (own, ry_c.at[layer]), 2 * rows)
        swap_x(layer).start()

    def final(layer):
        for color in range(2):
            pool = pools[color]
            up = line(layer, color, pz, "u")
            down = line(layer, color, pz, "d")
            own = pool.at[layer, 2 * nz + pz]
            from_up = pool.at[layer, 3 * nz + pz]
            from_down = pool.at[layer, 4 * nz + pz]
            target = out_at(layer, color)

            @pl.when(pz == 0)
            def _():
                down.wait_recv()
                add(target, (own, from_down))

            @pl.when(pz == nz - 1)
            def _():
                up.wait_recv()
                add(target, (own, from_up))

            @pl.when(jnp.logical_and(pz > 0, pz < nz - 1))
            def _():
                down.wait_recv()
                up.wait_recv()
                add(target, (own, from_up, from_down))

        swap_x(layer).wait_recv()
        own = ry_c.at[layer, pl.ds(pl.multiple_of(px * rows, 16), rows), :]
        add(out_at(layer, 2), (own, rx_c.at[layer]))

    def drain(layer):
        for z in zs:
            for color in range(2):
                hop_one(layer, color, 1, z).wait_send()
                hop_one(layer, color, 0, z).wait_send()
                hop_two(layer, color, z).wait_send()
                pl.when(pz < z)(lambda c=color, z=z: line(layer, c, z, "u").wait_send())
                pl.when(pz > z)(lambda c=color, z=z: line(layer, c, z, "d").wait_send())
            pl.when(pz < z)(lambda z=z: line_c(layer, z, "u", False).wait_send())
            pl.when(pz > z)(lambda z=z: line_c(layer, z, "d", False).wait_send())
        swap_y(layer).wait_send()
        swap_x(layer).wait_send()

    def fill(color):
        first, width = spans[color]
        fill_products(pairs, vector_rows, part, first, first + width)

    fill(0)
    fill(1)
    issue(zs[0])
    fill(2)
    if nz > 1:
        issue(zs[1])
    start_c(0)
    for i in range(nz + 2):
        if i < nz:
            second(0, zs[i])
        if i + 2 < nz:
            issue(zs[i + 2])
        if 1 <= i <= nz:
            relay_c(0, zs[i - 1])
        if i == nz:
            settle_c(0)
        if 1 <= i <= nz:
            third(0, zs[i - 1])
        if i >= 2:
            relay(0, zs[i - 2])
    x_c(0)
    final(0)
    drain(0)


def sum_rows(pairs, vector_rows, nz):
    layers = 1
    depth = pairs[0][0].shape[1]
    cols = sum(right.shape[1] for _, right in pairs) + vector_rows.shape[0]
    n = 4 * nz
    rows = depth // n
    spans = split_columns(cols)
    vmem = pl.BlockSpec(memory_space=pltpu.VMEM)
    dt = jnp.bfloat16
    count = 12 * nz + 2
    heads_wide = pairs[1][1].shape[1]
    ff_wide = pairs[-1][1].shape[1]
    return pl.pallas_call(
        functools.partial(sum_kernel, nz, len(pairs), rows, cols),
        out_shape=(
            jax.ShapeDtypeStruct((LAYERS, rows, 3, heads_wide), jnp.float32),
            jax.ShapeDtypeStruct((LAYERS, heads_wide, rows), jnp.float32),
            jax.ShapeDtypeStruct((rows, ff_wide), jnp.float32),
            jax.ShapeDtypeStruct((ff_wide, rows), jnp.float32),
            jax.ShapeDtypeStruct((rows, vector_rows.shape[0]), jnp.float32),
        ),
        in_specs=[vmem] * (2 * len(pairs) + 1),
        out_specs=(vmem,) * 5,
        scratch_shapes=[
            pltpu.VMEM((depth, cols), dt),
            pltpu.VMEM((layers, 5 * nz, rows, spans[0][1]), dt),
            pltpu.VMEM((layers, 5 * nz, rows, spans[1][1]), dt),
            pltpu.VMEM((layers, 2 * nz, 4 * rows, spans[2][1]), dt),
            pltpu.VMEM((layers, 2 * rows, spans[2][1]), dt),
            pltpu.VMEM((layers, rows, spans[2][1]), dt),
            pltpu.VMEM((layers, 4 * rows, spans[2][1]), dt),
            pltpu.SemaphoreType.DMA((layers, count)),
            pltpu.SemaphoreType.DMA((layers, count)),
            pltpu.VMEM((rows, cols), jnp.float32),
        ],
        compiler_params=pltpu.CompilerParams(
            collective_id=1, has_side_effects=True, vmem_limit_bytes=60 * 1024 * 1024
        ),
        name="sum_rows",
    )(*[side for pair in pairs for side in pair], vector_rows)


def scaled_scores(q, k, same):
    scores = mul(q, k, ((1,), (1,))) * SCORE_SCALE
    return jnp.where(same, scores, MASK_FILL)


def pair_at(first, offset):
    return pl.ds(pl.multiple_of(first + offset, LANES), LANES)


def attention_kernel(chunk, joined, seg_col, seg_row, context, log_total):
    length, cols = context.shape
    lane = lax.broadcasted_iota(jnp.int32, (chunk, LANES), 1)
    for start in range(0, length, chunk):
        at = pl.ds(start, chunk)
        log_total[at, :] = jnp.zeros((chunk, LANES), jnp.float32)

    def pair(i, carry):
        first = i * LANES
        k_pair = joined[:, pair_at(first, cols)]
        v_pair = joined[:, pair_at(first, 2 * cols)]
        for start in range(0, length, chunk):
            at = pl.ds(start, chunk)
            same = seg_col[at, :] == seg_row[...]
            q_pair = joined[at, pair_at(first, 0)]
            logs = log_total[at, :]
            made = []
            for which, low in enumerate(range(0, LANES, HEAD_DIM)):
                part = slice(low, low + HEAD_DIM)
                scores = scaled_scores(q_pair[:, part], k_pair[:, part], same)
                top = jnp.max(scores, axis=1, keepdims=True)
                exponent = jnp.exp(scores - top)
                total = jnp.sum(exponent, axis=1, keepdims=True)
                probs = (exponent / total).astype(jnp.bfloat16)
                made.append(mul(probs, v_pair[:, part], ((1,), (0,))))
                head = i * (LANES // HEAD_DIM) + which
                logs = jnp.where(lane == head, top + jnp.log(total), logs)
            context[at, pair_at(first, 0)] = jnp.concatenate(made, axis=1).astype(jnp.bfloat16)
            log_total[at, :] = logs
        return carry

    lax.fori_loop(0, cols // LANES, pair, 0)


def attention_back_kernel(
    chunk, joined, context_low, log_total, seg_col, seg_row, joined_grad, column_sums
):
    length, cols = context_low.shape
    lane = lax.broadcasted_iota(jnp.int32, (chunk, LANES), 1)

    def pair(i, carry):
        first = i * LANES
        k_pair = joined[:, pair_at(first, cols)]
        v_pair = joined[:, pair_at(first, 2 * cols)]
        key_sums = [None] * (LANES // HEAD_DIM)
        value_sums = [None] * (LANES // HEAD_DIM)
        query_column = jnp.zeros((1, LANES), jnp.float32)
        for start in range(0, length, chunk):
            at = pl.ds(start, chunk)
            same = seg_col[at, :] == seg_row[...]
            q_pair = joined[at, pair_at(first, 0)]
            c_pair = context_low[at, pair_at(first, 0)]
            logs = log_total[at, :]
            made = []
            for which, low in enumerate(range(0, LANES, HEAD_DIM)):
                part = slice(low, low + HEAD_DIM)
                q, k, v, c = q_pair[:, part], k_pair[:, part], v_pair[:, part], c_pair[:, part]
                head = i * (LANES // HEAD_DIM) + which
                log_sum = jnp.sum(jnp.where(lane == head, logs, 0.0), axis=1, keepdims=True)
                probabilities = jnp.exp(scaled_scores(q, k, same) - log_sum)
                prob_grad = mul(c, v, ((1,), (1,)))
                row_delta = jnp.sum(prob_grad * probabilities, axis=1, keepdims=True)
                score_grad = (probabilities * (prob_grad - row_delta)).astype(jnp.bfloat16)
                value_part = mul(probabilities.astype(jnp.bfloat16), c, ((0,), (0,)))
                key_part = mul(score_grad, q, ((0,), (0,)))
                made.append(mul(score_grad, k, ((1,), (0,))))
                if start:
                    value_part = value_part + value_sums[which]
                    key_part = key_part + key_sums[which]
                value_sums[which] = value_part
                key_sums[which] = key_part
            query_grad = (jnp.concatenate(made, axis=1) * SCORE_SCALE).astype(jnp.bfloat16)
            joined_grad[at, pair_at(first, 0)] = query_grad
            query_column = query_column + jnp.sum(
                query_grad.astype(jnp.float32), axis=0, keepdims=True
            )
        key_grad = (jnp.concatenate(key_sums, axis=1) * SCORE_SCALE).astype(jnp.bfloat16)
        value_grad = jnp.concatenate(value_sums, axis=1).astype(jnp.bfloat16)
        joined_grad[:, pair_at(first, cols)] = key_grad
        joined_grad[:, pair_at(first, 2 * cols)] = value_grad
        column_sums[0:1, pair_at(first, 0)] = query_column
        column_sums[1:2, pair_at(first, 0)] = jnp.sum(
            value_grad.astype(jnp.float32), axis=0, keepdims=True
        )
        return carry

    lax.fori_loop(0, cols // LANES, pair, 0)


def local_kernel(body, shapes, work, name, *arrays):
    vmem = pl.BlockSpec(memory_space=pltpu.VMEM)
    return pl.pallas_call(
        body,
        out_shape=shapes,
        in_specs=[vmem] * len(arrays),
        out_specs=tuple(vmem for _ in shapes),
        compiler_params=pltpu.CompilerParams(vmem_limit_bytes=40 * 1024 * 1024),
        cost_estimate=pl.CostEstimate(flops=work, bytes_accessed=1 << 22, transcendentals=1 << 21),
        name=name,
    )(*arrays)


def pair_sum(rows, tp_rank):
    layers, depth, cols = rows.shape
    halves = rows.reshape(layers, 2, depth // 2, cols)
    away = lax.dynamic_index_in_dim(halves, 1 - tp_rank, 1, keepdims=False)
    mine = lax.dynamic_index_in_dim(halves, tp_rank, 1, keepdims=False)
    return mine + lax.ppermute(away, "tp", [(0, 1), (1, 0)])


def per_device(
    block_input,
    cotangent,
    qkv_weight,
    proj_weight,
    fc1_weight,
    fc2_weight,
    norm_gains,
    biases,
    fc1_bias,
    segments,
    keep_flags,
):
    local_len, row_count, width = block_input.shape
    assert row_count == 1
    tp_rank = lax.axis_index("tp")
    tp_size = lax.axis_size("tp")
    full_len = local_len * tp_size
    shard_rows = qkv_weight.shape[1]
    head_cols = qkv_weight.shape[3]
    ff_cols = fc1_weight.shape[2]
    qkv_end = 3 * head_cols
    proj_end = qkv_end + head_cols
    fc1_end = proj_end + ff_cols
    bf16 = jnp.bfloat16
    f32 = jnp.float32

    segment_row = segments[0]
    local_segments = lax.dynamic_slice_in_dim(segment_row, tp_rank * local_len, local_len, 0)
    member = (
        local_segments[:, None] == jnp.arange(SEGS, dtype=jnp.int32)[None, :]
    ).astype(f32)

    def token_keep(keep_row):
        return jnp.sum(member * keep_row.astype(f32), axis=1, keepdims=True)

    def place(part_grad, total_len):
        return lax.dynamic_update_slice_in_dim(
            jnp.zeros((total_len,), f32), part_grad, tp_rank * part_grad.shape[0], 0
        )

    def gather_positions(local_rows):
        return lax.all_gather(local_rows, "tp", axis=0, tiled=True)

    def scatter_positions(partial):
        if tp_size == 2:
            halves = partial.reshape(2, local_len, width)
            away = lax.dynamic_index_in_dim(halves, 1 - tp_rank, 0, keepdims=False)
            mine = lax.dynamic_index_in_dim(halves, tp_rank, 0, keepdims=False)
            arrived = lax.ppermute(away, "tp", [(0, 1), (1, 0)])
            return mine.astype(f32) + arrived.astype(f32)
        return lax.psum_scatter(partial, "tp", scatter_dimension=0, tiled=True).astype(f32)

    row_devices = lax.axis_size("rows")
    own_kernels = shard_rows % 16 == 0 and row_devices % 4 == 0 and tp_size == 2
    shards = (
        [
            jnp.concatenate(
                [
                    qkv_weight[layer].reshape(shard_rows, qkv_end).astype(bf16),
                    proj_weight[layer].T.astype(bf16),
                    fc1_weight[layer].astype(bf16),
                    fc2_weight[layer].T.astype(bf16),
                ],
                axis=1,
            )
            for layer in range(LAYERS)
        ]
    )
    vector_parts = [norm_gains, biases, fc1_bias[:, None, :]]
    vector_flat = jnp.concatenate([part.reshape(-1) for part in vector_parts])
    if own_kernels:
        filled = -(-vector_flat.size // (8 * LANES)) * 8 * LANES
        packed_first, vector_full = gather_rows(
            shards[0][None],
            jnp.pad(vector_flat, (0, filled - vector_flat.size)).reshape(-1, LANES),
            row_devices // 4,
        )
        vector_full = vector_full.reshape(row_devices * tp_size, -1)
        packed_full = [packed_first[0]] + [
            lax.all_gather(shard, "rows", axis=0, tiled=True) for shard in shards[1:]
        ]
    else:
        packed_full = [lax.all_gather(shard, "rows", axis=0, tiled=True) for shard in shards]
        vector_full = lax.all_gather(vector_flat, ("rows", "tp"), axis=0, tiled=False)
    full_vectors = []
    first = 0
    for part in vector_parts:
        taken = vector_full[:, first : first + part.size].reshape((-1,) + part.shape)
        first += part.size
        full_vectors.append(jnp.moveaxis(taken, 0, 2).reshape(part.shape[0], part.shape[1], -1))
    gains_full, biases_full, fc1_bias_full = full_vectors

    stream = block_input[:, 0]
    saved = []
    for layer in range(LAYERS):
        packed = packed_full[layer]
        w_qkv = packed[:, :qkv_end]
        w_proj = packed[:, qkv_end:proj_end]
        w_fc1 = packed[:, proj_end:fc1_end]
        w_fc2 = packed[:, fc1_end:]
        gain = gains_full[layer]
        bias = biases_full[layer]
        in_bias = jnp.concatenate(
            [
                lax.dynamic_slice_in_dim(bias[1], tp_rank * head_cols, head_cols, 0),
                jnp.zeros((head_cols,), f32),
                lax.dynamic_slice_in_dim(bias[2], tp_rank * head_cols, head_cols, 0),
            ]
        )
        up_bias = lax.dynamic_slice_in_dim(fc1_bias_full[layer, 0], tp_rank * ff_cols, ff_cols, 0)
        keep_attn = token_keep(keep_flags[layer, 0])
        keep_mlp = token_keep(keep_flags[layer, 1])
        xhat_one, rstd_one = apply_layer_norm(stream)
        normed_one = gather_positions((xhat_one * gain[0] + bias[0]).astype(bf16))
        joined = (mul(normed_one, w_qkv, ((1,), (0,))) + in_bias).astype(bf16)
        context, log_total = local_kernel(
            functools.partial(attention_kernel, full_len // 2),
            (
                jax.ShapeDtypeStruct((full_len, head_cols), bf16),
                jax.ShapeDtypeStruct((full_len, LANES), f32),
            ),
            4 * full_len * full_len * head_cols,
            "attention",
            joined,
            segment_row[:, None],
            segment_row[None],
        )
        attn = scatter_positions(mul(context, w_proj, ((1,), (1,))).astype(bf16)) + bias[3]
        middle = stream + keep_attn * attn / KEEP_RATE
        xhat_two, rstd_two = apply_layer_norm(middle)
        normed_two = gather_positions((xhat_two * gain[1] + bias[4]).astype(bf16))
        hidden_pre = mul(normed_two, w_fc1, ((1,), (0,))) + up_bias
        hidden = (hidden_pre * cumulative(hidden_pre)).astype(bf16)
        mlp = scatter_positions(mul(hidden, w_fc2, ((1,), (1,))).astype(bf16)) + bias[5]
        stream = middle + keep_mlp * mlp / KEEP_RATE
        saved.append(
            (
                (w_qkv, w_proj, w_fc1, w_fc2, gain, keep_attn, keep_mlp),
                (xhat_one, rstd_one, normed_one, joined, log_total, context),
                (xhat_two, rstd_two, normed_two, hidden_pre, hidden),
            )
        )

    grad = cotangent[:, 0]
    early_sums = [None] * LAYERS
    late_pairs = []
    all_vectors = []
    for layer in reversed(range(LAYERS)):
        (w_qkv, w_proj, w_fc1, w_fc2, gain, keep_attn, keep_mlp), attn_side, mlp_side = saved[layer]
        xhat_one, rstd_one, normed_one, joined, log_total, context = attn_side
        xhat_two, rstd_two, normed_two, hidden_pre, hidden = mlp_side
        mlp_grad = grad * keep_mlp / KEEP_RATE
        fc2_bias_grad = jnp.sum(mlp_grad, axis=0)
        mlp_low = gather_positions(mlp_grad.astype(bf16))
        hidden_grad = mul(mlp_low, w_fc2, ((1,), (0,)))
        pre_grad = (hidden_grad * gelu_slope(hidden_pre)).astype(bf16)
        if layer:
            packed = pack_products([(normed_two, pre_grad), (mlp_low, hidden)])
            packed, pre_grad = lax.optimization_barrier((packed, pre_grad))
            early_sums[layer] = lax.psum_scatter(
                packed, "rows", scatter_dimension=0, tiled=True
            ).astype(f32)
        fc1_bias_grad = jnp.sum(pre_grad.astype(f32), axis=0)
        two_grad = scatter_positions(mul(pre_grad, w_fc1, ((1,), (1,))).astype(bf16))
        gain_two_grad = jnp.sum(two_grad * xhat_two, axis=0)
        shift_two_grad = jnp.sum(two_grad, axis=0)
        middle_grad = grad + norm_backward(two_grad, xhat_two, rstd_two, gain[1])
        attn_grad = middle_grad * keep_attn / KEEP_RATE
        proj_bias_grad = jnp.sum(attn_grad, axis=0)
        attn_low = gather_positions(attn_grad.astype(bf16))
        context_low = mul(attn_low, w_proj, ((1,), (0,))).astype(bf16)
        joined_grad, in_bias_grad = local_kernel(
            functools.partial(attention_back_kernel, full_len // 2),
            (
                jax.ShapeDtypeStruct((full_len, 3 * head_cols), bf16),
                jax.ShapeDtypeStruct((2, head_cols), f32),
            ),
            10 * full_len * full_len * head_cols,
            "attention_back",
            joined,
            context_low,
            log_total,
            segment_row[:, None],
            segment_row[None],
        )
        one_grad = scatter_positions(mul(joined_grad, w_qkv, ((1,), (1,))).astype(bf16))
        gain_one_grad = jnp.sum(one_grad * xhat_one, axis=0)
        shift_one_grad = jnp.sum(one_grad, axis=0)
        grad = middle_grad + norm_backward(one_grad, xhat_one, rstd_one, gain[0])
        all_vectors += [
            gain_one_grad[None],
            gain_two_grad[None],
            shift_one_grad[None],
            place(in_bias_grad[0], width)[None],
            place(in_bias_grad[1], width)[None],
            proj_bias_grad[None],
            shift_two_grad[None],
            fc2_bias_grad[None],
            place(fc1_bias_grad, ff_cols * tp_size).reshape(width, -1).T,
        ]
        late_pairs += [(normed_one, joined_grad), (attn_low, context)]
        if not layer:
            late_pairs += [(normed_two, pre_grad), (mlp_low, hidden)]

    vector_count = 8 + ff_cols * tp_size // width
    vector_rows = jnp.concatenate(all_vectors, axis=0)
    vector_rows = jnp.pad(vector_rows, ((0, LANES - vector_rows.shape[0]), (0, 0)))
    if own_kernels:
        qkv_out, proj_out, fc1_late, fc2_late, late_vectors = sum_rows(
            late_pairs, vector_rows, row_devices // 4
        )
    else:
        late_sum = lax.psum_scatter(
            pack_products(late_pairs, vector_rows), "rows", scatter_dimension=0, tiled=True
        ).astype(f32)
        both_layers = [
            late_sum[:, layer * proj_end : (layer + 1) * proj_end]
            for layer in reversed(range(LAYERS))
        ]
        qkv_out = jnp.stack(
            [part[:, :qkv_end].reshape(shard_rows, 3, head_cols) for part in both_layers]
        )
        proj_out = jnp.stack([part[:, qkv_end:].T for part in both_layers])
        rest = late_sum[:, LAYERS * proj_end :]
        fc1_late = rest[:, :ff_cols]
        fc2_late = rest[:, ff_cols : 2 * ff_cols].T
        late_vectors = rest[:, 2 * ff_cols :]
    fc1_out = jnp.stack([fc1_late] + [part[:, :ff_cols] for part in early_sums[1:]])
    fc2_out = jnp.stack([fc2_late] + [part[:, ff_cols:].T for part in early_sums[1:]])
    late_vectors = late_vectors[None]
    if tp_size == 2:
        late_vectors = pair_sum(late_vectors, tp_rank)[0]
    else:
        late_vectors = lax.psum_scatter(
            late_vectors, "tp", scatter_dimension=1, tiled=True
        )[0]
    vector_sums = [
        late_vectors[:, layer * vector_count : (layer + 1) * vector_count]
        for layer in reversed(range(LAYERS))
    ]
    return (
        stream[:, None],
        grad[:, None],
        qkv_out,
        proj_out,
        fc1_out,
        fc2_out,
        jnp.stack([part[:, :2].T for part in vector_sums]),
        jnp.stack([part[:, 2:8].T for part in vector_sums]),
        jnp.stack([part[:, 8:].reshape(-1) for part in vector_sums]),
    )


def solution(mesh):
    placed = (
        P("tp", "rows", None),
        P("tp", "rows", None),
        P(None, "rows", None, "tp"),
        P(None, "tp", "rows"),
        P(None, "rows", "tp"),
        P(None, "tp", "rows"),
        P(None, None, ("rows", "tp")),
        P(None, None, ("rows", "tp")),
        P(None, ("rows", "tp")),
        P("rows", None),
        P(None, None, "rows", None),
    )
    return jax.shard_map(
        per_device,
        mesh=mesh,
        in_specs=placed,
        out_specs=placed[:2] + placed[2:9],
        check_vma=False,
    )
```

```python
import functools
import math

import jax
import jax.numpy as jnp
from jax import lax
from jax.experimental import pallas as pl
from jax.experimental.pallas import tpu as pltpu
from jax.sharding import PartitionSpec as P


MESH = pl.DeviceIdType.MESH
LANES = 128
GATHER_ORDERS = ("zyx", "zxy", "xyz")
HEAD_DIM = 64
LAYERS = 2
SEGS = 8

NORM_EPS = 1e-06
KEEP_RATE = 0.9
SCORE_SCALE = 0.125
MASK_FILL = -1e30
INV_SQRT_TWO = 1.0 / math.sqrt(2.0)
INV_SQRT_TWO_PI = 1.0 / math.sqrt(2.0 * math.pi)


def apply_layer_norm(residual_rows):
    center = residual_rows - jnp.mean(residual_rows, axis=-1, keepdims=True)
    spread = jnp.mean(center * center, axis=-1, keepdims=True)
    inverse_deviation = lax.rsqrt(spread + NORM_EPS)
    return (center * inverse_deviation, inverse_deviation)


def norm_backward(normed_gradient, centered_unit, inverse_deviation, norm_gain):
    scaled_rows = normed_gradient * norm_gain
    return inverse_deviation * (
        scaled_rows
        - jnp.mean(scaled_rows, axis=-1, keepdims=True)
        - centered_unit * jnp.mean(scaled_rows * centered_unit, axis=-1, keepdims=True)
    )


def cumulative(u):
    return 0.5 * (1.0 + lax.erf(u * INV_SQRT_TWO))


def gelu_slope(u):
    return cumulative(u) + u * jnp.exp(-0.5 * u * u) * INV_SQRT_TWO_PI


def mul(a, b, dims):
    return lax.dot_general(a, b, (dims, ((), ())), preferred_element_type=jnp.float32)


def split_columns(total):
    groups = total // LANES
    first = groups * 14 // 36
    return (
        (0, first * LANES),
        (first * LANES, first * LANES),
        (2 * first * LANES, (groups - 2 * first) * LANES),
    )


def places(nz):
    me = lax.axis_index("rows")
    px = lax.rem(me, 2)
    py = lax.rem(lax.div(me, 2), 2)
    pz = lax.div(me, 4)
    hops = {
        "x": me + 1 - 2 * px,
        "y": me + 2 - 4 * py,
        "u": lax.min(me + 4, 4 * nz - 1),
        "d": lax.max(me - 4, 0),
    }
    return me, px, py, pz, hops


def guarded(cond, act):
    if cond is None:
        act()
    else:
        pl.when(cond)(act)


def both(a, b):
    if a is None:
        return b
    if b is None:
        return a
    return jnp.logical_and(a, b)


def greet(nz, pz, hops, tp, with_tp):
    barrier = pltpu.get_barrier_semaphore()
    ends = {"x": None, "y": None, "u": pz < nz - 1, "d": pz > 0}
    for name, cond in ends.items():
        guarded(
            cond,
            lambda name=name: pl.semaphore_signal(
                barrier, inc=1, device_id=(hops[name], tp), device_id_type=MESH
            ),
        )
    waits = 2
    if with_tp:
        pl.semaphore_signal(
            barrier, inc=1, device_id=(lax.axis_index("rows"), 1 - tp), device_id_type=MESH
        )
        waits = 3
    waits = waits + lax.min(pz, 1) + lax.min(nz - 1 - pz, 1)
    pl.semaphore_wait(barrier, waits)
    return ends


def gather_plan(order, nz):
    found = []
    for rx in (0, 1):
        for ry in (0, 1):
            for rz in range(1 - nz, nz):
                rel = {"x": rx, "y": ry, "z": rz}
                differing = [i for i, dim in enumerate(order) if rel[dim]]
                last = differing[-1] if differing else -1
                sends = []
                if last >= 0 and order[last] == "z":
                    sends.append("u" if rz < 0 else "d")
                for dim in order[last + 1 :]:
                    sends.extend("ud" if dim == "z" else dim)
                found.append((last + 1, abs(rz), rx + ry, rx, ry, rz, tuple(sends)))
    return sorted(found)


def gather_kernel(nz, layers, rows, cols, shard, vec, full, vec_full, own_sem, recv, send):
    me, px, py, pz, hops = places(nz)
    tp = lax.axis_index("tp")
    n = 4 * nz
    spans = split_columns(cols)
    names = "xyud"
    ends = greet(nz, pz, hops, tp, True)

    def origin(rx, ry, rz):
        return me + rx * (1 - 2 * px) + ry * 2 * (1 - 2 * py) + 4 * rz

    def block(layer, color, o):
        start = pl.multiple_of((layer * n + o) * rows, 16)
        return full.at[pl.ds(start, rows), pl.ds(*spans[color])]

    def copy(layer, color, o, name, own):
        if color == 3:
            src = vec_full.at[o]
            dst = vec_full.at[o]
        else:
            dst = block(layer, color, o)
            src = dst
            if own:
                start = pl.multiple_of(layer * rows, 16)
                src = shard.at[pl.ds(start, rows), pl.ds(*spans[color])]
        return pltpu.make_async_remote_copy(
            src_ref=src,
            dst_ref=dst,
            send_sem=send.at[layer, color, names.index(name), o],
            recv_sem=recv.at[layer, color, o],
            device_id=(hops[name], tp),
            device_id_type=MESH,
        )

    keep = pltpu.make_async_copy(vec, vec_full.at[me, tp], own_sem.at[0])
    keep.start()
    swap = pltpu.make_async_remote_copy(
        src_ref=vec,
        dst_ref=vec_full.at[me, tp],
        send_sem=own_sem.at[1],
        recv_sem=own_sem.at[2],
        device_id=(me, 1 - tp),
        device_id_type=MESH,
    )
    swap.start()
    plans = [gather_plan(order, nz) for order in GATHER_ORDERS + ("xyz",)]

    def visit(layer, color, item, waiting):
        _, _, _, rx, ry, rz, sends = item
        o = origin(rx, ry, rz)
        own = (rx, ry, rz) == (0, 0, 0)
        valid = None if rz == 0 else jnp.logical_and(pz + rz >= 0, pz + rz < nz)

        def act():
            if not waiting and not own:
                name = "x"
                copy(layer, color, o, name, False).wait_recv()
            for name in sends:

                def go(name=name):
                    c = copy(layer, color, o, name, own)
                    if waiting:
                        c.wait_send()
                    else:
                        c.start()

                guarded(ends[name], go)

        guarded(valid, act)

    def own_place(layer):
        src = shard.at[pl.ds(pl.multiple_of(layer * rows, 16), rows), :]
        dst = full.at[pl.ds(pl.multiple_of((layer * n + me) * rows, 16), rows), :]
        return pltpu.make_async_copy(src, dst, own_sem.at[3 + layer])

    for phase in range(4):
        stacks = [[item for item in plan if item[0] == phase] for plan in plans]

        def step(layer, carry):
            for i in range(max(len(s) for s in stacks[:3])):
                for color in range(3):
                    if i < len(stacks[color]):
                        visit(layer, color, stacks[color][i], False)
            return carry

        lax.fori_loop(0, layers, step, 0)
        if phase == 0:
            lax.fori_loop(0, layers, lambda layer, c: (own_place(layer).start(), c)[1], 0)
            keep.wait()
            swap.wait()
        for item in stacks[3]:
            visit(0, 3, item, False)

    def finish(layer, carry):
        for color in range(3):
            for item in plans[color]:
                visit(layer, color, item, True)
        own_place(layer).wait()
        return carry

    lax.fori_loop(0, layers, finish, 0)
    for item in plans[3]:
        visit(0, 3, item, True)


def gather_rows(shards, vec, nz):
    layers, rows, cols = shards.shape
    n = 4 * nz
    any_space = pl.BlockSpec(memory_space=pl.ANY)
    vmem = pl.BlockSpec(memory_space=pltpu.VMEM)
    full, vec_full = pl.pallas_call(
        functools.partial(gather_kernel, nz, layers, rows, cols),
        out_shape=(
            jax.ShapeDtypeStruct((layers * n * rows, cols), shards.dtype),
            jax.ShapeDtypeStruct((n, 2) + vec.shape, vec.dtype),
        ),
        in_specs=[vmem, vmem],
        out_specs=(any_space, any_space),
        scratch_shapes=[
            pltpu.SemaphoreType.DMA((3 + layers,)),
            pltpu.SemaphoreType.DMA((layers, 4, n)),
            pltpu.SemaphoreType.DMA((layers, 4, 4, n)),
        ],
        compiler_params=pltpu.CompilerParams(
            collective_id=0, has_side_effects=True, vmem_limit_bytes=8 * 1024 * 1024
        ),
        name="gather_rows",
    )(shards.reshape(layers * rows, cols), vec)
    return full.reshape(layers, n * rows, cols), vec_full


def product_tiles(pairs, first, end):
    tiles = []
    at = 0
    for which, (_, right) in enumerate(pairs):
        width = right.shape[1]
        start = max(first, at)
        while start < min(end, at + width):
            size = min(512, min(end, at + width) - start)
            tiles.append((which, start - at, start, size))
            start += size
        at += width
    return tiles, at


def fill_products(pairs, vector_rows, part, first, end):
    tiles, products_end = product_tiles(pairs, first, end)
    for which, at, to, size in tiles:
        left, right = pairs[which]
        part[:, to : to + size] = lax.dot_general(
            left[...],
            right[:, at : at + size],
            (((0,), (0,)), ((), ())),
            preferred_element_type=jnp.float32,
        ).astype(part.dtype)
    if end > products_end:
        part[:, products_end:end] = vector_rows[...].T.astype(part.dtype)


def pack_kernel(count, *refs):
    part = refs[-1]
    pairs = [(refs[2 * i], refs[2 * i + 1]) for i in range(count)]
    fill_products(pairs, refs[2 * count], part, 0, part.shape[1])


def pack_products(pairs, vector_rows=None):
    depth = pairs[0][0].shape[1]
    cols = sum(right.shape[1] for _, right in pairs)
    operands = [side for pair in pairs for side in pair]
    if vector_rows is not None:
        cols += vector_rows.shape[0]
        operands.append(vector_rows)
    vmem = pl.BlockSpec(memory_space=pltpu.VMEM)
    flops = 2 * pairs[0][0].shape[0] * depth * cols
    return pl.pallas_call(
        functools.partial(pack_kernel, len(pairs)),
        out_shape=jax.ShapeDtypeStruct((depth, cols), jnp.bfloat16),
        in_specs=[vmem] * len(operands),
        out_specs=vmem,
        compiler_params=pltpu.CompilerParams(vmem_limit_bytes=40 * 1024 * 1024),
        cost_estimate=pl.CostEstimate(
            flops=flops, bytes_accessed=2 * depth * cols, transcendentals=0
        ),
        name="pack_products",
    )(*operands)


def sum_kernel(nz, count, rows, cols, *refs):
    pairs = [(refs[2 * i], refs[2 * i + 1]) for i in range(count)]
    vector_rows = refs[2 * count]
    outs = refs[2 * count + 1 : 2 * count + 6]
    part, ra, rb, rc, ry_c, rx_c, sc, send, recv, out = refs[2 * count + 6 :]
    sum_body(
        nz, 1, rows, cols, pairs, vector_rows, part, out,
        ra, rb, rc, ry_c, rx_c, sc, send, recv,
    )
    qkv_out, proj_out, fc1_out, fc2_out, vector_out = outs
    at = 0
    for layer in reversed(range(LAYERS)):
        for kind in range(3):
            wide = qkv_out.shape[3]
            qkv_out[layer, kind] = out[:, at : at + wide]
            at += wide
        wide = proj_out.shape[2]
        proj_out[layer] = out[:, at : at + wide]
        at += wide
    wide = fc1_out.shape[1]
    fc1_out[...] = out[:, at : at + wide]
    fc2_out[...] = out[:, at + wide : at + 2 * wide]
    vector_out[...] = out[:, at + 2 * wide :]


def sum_body(nz, layers, rows, cols, pairs, vector_rows, part, out, ra, rb, rc, ry_c, rx_c, sc, send, recv):
    me, px, py, pz, hops = places(nz)
    tp = lax.axis_index("tp")
    n = 4 * nz
    spans = split_columns(cols)
    ends = greet(nz, pz, hops, tp, False)
    base = (0, 5 * nz, 10 * nz)
    pools = (ra, rb)
    coord = {"x": px, "y": py}
    stride = {"x": 1, "y": 2}
    zs = []
    for k in range((nz + 1) // 2):
        zs.extend([nz - 1 - k, k] if nz - 1 - k != k else [k])

    def mine(layer, o, color, count=1):
        start = pl.multiple_of((layer * n + o) * rows, 16)
        return part.at[pl.ds(start, count * rows), pl.ds(*spans[color])]

    def copy(src, dst, layer, index, name):
        return pltpu.make_async_remote_copy(
            src_ref=src,
            dst_ref=dst,
            send_sem=send.at[layer, index],
            recv_sem=recv.at[layer, index],
            device_id=(hops[name], tp),
            device_id_type=MESH,
        )

    def add(dst, sources, count=rows):
        def chunk(i, carry):
            at = pl.ds(pl.multiple_of(i * 16, 16), 16)
            total = sources[0][at, :].astype(jnp.float32)
            for s in sources[1:]:
                total = total + s[at, :].astype(jnp.float32)
            dst[at, :] = total.astype(dst.dtype)
            return carry

        lax.fori_loop(0, count // 16, chunk, 0)

    dims = (("x", "y"), ("y", "x"))

    def dest(color, flip_one, flip_two, z):
        d1, d2 = dims[color]
        c1 = coord[d1] if not flip_one else 1 - coord[d1]
        c2 = coord[d2] if not flip_two else 1 - coord[d2]
        return 4 * z + stride[d1] * c1 + stride[d2] * c2

    def hop_one(layer, color, flip_two, z):
        slot = flip_two * nz + z
        dst = pools[color].at[layer, slot]
        return copy(
            mine(layer, dest(color, 1, flip_two, z), color),
            dst,
            layer,
            base[color] + slot,
            dims[color][0],
        )

    def hop_two(layer, color, z):
        pool = pools[color]
        slot = 2 * nz + z
        return copy(
            pool.at[layer, nz + z], pool.at[layer, slot], layer, base[color] + slot, dims[color][1]
        )

    def line(layer, color, z, name):
        pool = pools[color]
        slot = (3 if name == "u" else 4) * nz + z
        return copy(
            pool.at[layer, 2 * nz + z], pool.at[layer, slot], layer, base[color] + slot, name
        )

    def line_c(layer, z, name, direct):
        slot = (0 if name == "u" else nz) + z
        dst = rc.at[layer, slot]
        src = mine(layer, 4 * z, 2, 4) if direct else dst
        return copy(src, dst, layer, base[2] + slot, name)

    def swap_y(layer):
        src = sc.at[layer, pl.ds(pl.multiple_of((1 - py) * 2 * rows, 16), 2 * rows), :]
        return copy(src, ry_c.at[layer], layer, base[2] + 2 * nz, "y")

    def swap_x(layer):
        src = ry_c.at[layer, pl.ds(pl.multiple_of((1 - px) * rows, 16), rows), :]
        return copy(src, rx_c.at[layer], layer, base[2] + 2 * nz + 1, "x")

    def issue(z, color):
        for flip in (1, 0):
            hop_one(0, color, flip, z).start()

    def start_c(layer):
        for z in zs:
            if z > 0:
                pl.when(pz == 0)(lambda z=z: line_c(layer, z, "u", True).start())
            if z < nz - 1:
                pl.when(pz == nz - 1)(lambda z=z: line_c(layer, z, "d", True).start())

    def relay_c(layer, z):
        if z > 1:

            @pl.when(jnp.logical_and(pz > 0, pz < z))
            def _():
                c = line_c(layer, z, "u", False)
                c.wait_recv()
                add(rc.at[layer, z], (mine(layer, 4 * z, 2, 4), rc.at[layer, z]), 4 * rows)
                c.start()

        if z < nz - 2:

            @pl.when(jnp.logical_and(pz < nz - 1, pz > z))
            def _():
                c = line_c(layer, z, "d", False)
                c.wait_recv()
                at = rc.at[layer, nz + z]
                add(at, (mine(layer, 4 * z, 2, 4), at), 4 * rows)
                c.start()

    def second(layer, z):
        for color in range(2):
            hop_one(layer, color, 1, z).wait_recv()
            at = pools[color].at[layer, nz + z]
            add(at, (mine(layer, dest(color, 0, 1, z), color), at))
            hop_two(layer, color, z).start()

    def settle_c(layer):
        up = line_c(layer, pz, "u", False)
        down = line_c(layer, pz, "d", False)
        own = mine(layer, 4 * pz, 2, 4)
        from_up = rc.at[layer, pz]
        from_down = rc.at[layer, nz + pz]
        target = sc.at[layer]

        @pl.when(pz == 0)
        def _():
            down.wait_recv()
            add(target, (own, from_down), 4 * rows)

        @pl.when(pz == nz - 1)
        def _():
            up.wait_recv()
            add(target, (own, from_up), 4 * rows)

        @pl.when(jnp.logical_and(pz > 0, pz < nz - 1))
        def _():
            down.wait_recv()
            up.wait_recv()
            add(target, (own, from_up, from_down), 4 * rows)

        swap_y(layer).start()

    def third(layer, z):
        for color in range(2):
            pool = pools[color]
            hop_one(layer, color, 0, z).wait_recv()
            hop_two(layer, color, z).wait_recv()
            at = pool.at[layer, 2 * nz + z]
            add(at, (mine(layer, dest(color, 0, 0, z), color), pool.at[layer, z], at))
            pl.when(jnp.logical_and(pz == 0, z > pz))(
                lambda color=color: line(layer, color, z, "u").start()
            )
            pl.when(jnp.logical_and(pz == nz - 1, z < pz))(
                lambda color=color: line(layer, color, z, "d").start()
            )

    def relay(layer, z):
        for color in range(2):
            pool = pools[color]
            at = pool.at[layer, 2 * nz + z]

            @pl.when(jnp.logical_and(pz > 0, pz < z))
            def _():
                c = line(layer, color, z, "u")
                c.wait_recv()
                add(at, (at, pool.at[layer, 3 * nz + z]))
                c.start()

            @pl.when(jnp.logical_and(pz < nz - 1, pz > z))
            def _():
                c = line(layer, color, z, "d")
                c.wait_recv()
                add(at, (at, pool.at[layer, 4 * nz + z]))
                c.start()

    def out_at(layer, color):
        return out.at[pl.ds(pl.multiple_of(layer * rows, 16), rows), pl.ds(*spans[color])]

    def x_c(layer):
        swap_y(layer).wait_recv()
        own = sc.at[layer, pl.ds(pl.multiple_of(py * 2 * rows, 16), 2 * rows), :]
        add(ry_c.at[layer], (own, ry_c.at[layer]), 2 * rows)
        swap_x(layer).start()

    def final(layer):
        for color in range(2):
            pool = pools[color]
            up = line(layer, color, pz, "u")
            down = line(layer, color, pz, "d")
            own = pool.at[layer, 2 * nz + pz]
            from_up = pool.at[layer, 3 * nz + pz]
            from_down = pool.at[layer, 4 * nz + pz]
            target = out_at(layer, color)

            @pl.when(pz == 0)
            def _():
                down.wait_recv()
                add(target, (own, from_down))

            @pl.when(pz == nz - 1)
            def _():
                up.wait_recv()
                add(target, (own, from_up))

            @pl.when(jnp.logical_and(pz > 0, pz < nz - 1))
            def _():
                down.wait_recv()
                up.wait_recv()
                add(target, (own, from_up, from_down))

        swap_x(layer).wait_recv()
        own = ry_c.at[layer, pl.ds(pl.multiple_of(px * rows, 16), rows), :]
        add(out_at(layer, 2), (own, rx_c.at[layer]))

    def drain(layer):
        for z in zs:
            for color in range(2):
                hop_one(layer, color, 1, z).wait_send()
                hop_one(layer, color, 0, z).wait_send()
                hop_two(layer, color, z).wait_send()
                pl.when(pz < z)(lambda c=color, z=z: line(layer, c, z, "u").wait_send())
                pl.when(pz > z)(lambda c=color, z=z: line(layer, c, z, "d").wait_send())
            pl.when(pz < z)(lambda z=z: line_c(layer, z, "u", False).wait_send())
            pl.when(pz > z)(lambda z=z: line_c(layer, z, "d", False).wait_send())
        swap_y(layer).wait_send()
        swap_x(layer).wait_send()

    def fill(color):
        first, width = spans[color]
        fill_products(pairs, vector_rows, part, first, first + width)

    fill(2)
    fill(0)
    start_c(0)
    for z in zs[:2]:
        issue(z, 0)
    fill(1)
    for z in zs[:2]:
        issue(z, 1)
    for i in range(nz + 2):
        if i < nz:
            second(0, zs[i])
        if i + 2 < nz:
            issue(zs[i + 2], 0)
            issue(zs[i + 2], 1)
        if 1 <= i <= nz:
            relay_c(0, zs[i - 1])
        if i == nz:
            settle_c(0)
        if 1 <= i <= nz:
            third(0, zs[i - 1])
        if i >= 2:
            relay(0, zs[i - 2])
    x_c(0)
    final(0)
    drain(0)


def sum_rows(pairs, vector_rows, nz):
    layers = 1
    depth = pairs[0][0].shape[1]
    cols = sum(right.shape[1] for _, right in pairs) + vector_rows.shape[0]
    n = 4 * nz
    rows = depth // n
    spans = split_columns(cols)
    vmem = pl.BlockSpec(memory_space=pltpu.VMEM)
    dt = jnp.bfloat16
    count = 12 * nz + 2
    heads_wide = pairs[1][1].shape[1]
    ff_wide = pairs[-1][1].shape[1]
    return pl.pallas_call(
        functools.partial(sum_kernel, nz, len(pairs), rows, cols),
        out_shape=(
            jax.ShapeDtypeStruct((LAYERS, 3, rows, heads_wide), jnp.float32),
            jax.ShapeDtypeStruct((LAYERS, rows, heads_wide), jnp.float32),
            jax.ShapeDtypeStruct((rows, ff_wide), jnp.float32),
            jax.ShapeDtypeStruct((rows, ff_wide), jnp.float32),
            jax.ShapeDtypeStruct((rows, vector_rows.shape[0]), jnp.float32),
        ),
        in_specs=[vmem] * (2 * len(pairs) + 1),
        out_specs=(vmem,) * 5,
        scratch_shapes=[
            pltpu.VMEM((depth, cols), dt),
            pltpu.VMEM((layers, 5 * nz, rows, spans[0][1]), dt),
            pltpu.VMEM((layers, 5 * nz, rows, spans[1][1]), dt),
            pltpu.VMEM((layers, 2 * nz, 4 * rows, spans[2][1]), dt),
            pltpu.VMEM((layers, 2 * rows, spans[2][1]), dt),
            pltpu.VMEM((layers, rows, spans[2][1]), dt),
            pltpu.VMEM((layers, 4 * rows, spans[2][1]), dt),
            pltpu.SemaphoreType.DMA((layers, count)),
            pltpu.SemaphoreType.DMA((layers, count)),
            pltpu.VMEM((rows, cols), jnp.float32),
        ],
        compiler_params=pltpu.CompilerParams(
            collective_id=1, has_side_effects=True, vmem_limit_bytes=60 * 1024 * 1024
        ),
        name="sum_rows",
    )(*[side for pair in pairs for side in pair], vector_rows)


def scaled_scores(q, k, same):
    scores = mul(q, k, ((1,), (1,))) * SCORE_SCALE
    return jnp.where(same, scores, MASK_FILL)


def pair_at(first, offset):
    return pl.ds(pl.multiple_of(first + offset, LANES), LANES)


def attention_kernel(chunk, joined, seg_col, seg_row, context, log_total):
    length, cols = context.shape
    lane = lax.broadcasted_iota(jnp.int32, (chunk, LANES), 1)
    for start in range(0, length, chunk):
        at = pl.ds(start, chunk)
        log_total[at, :] = jnp.zeros((chunk, LANES), jnp.float32)

    def pair(i, carry):
        first = i * LANES
        k_pair = joined[:, pair_at(first, cols)]
        v_pair = joined[:, pair_at(first, 2 * cols)]
        for start in range(0, length, chunk):
            at = pl.ds(start, chunk)
            same = seg_col[at, :] == seg_row[...]
            q_pair = joined[at, pair_at(first, 0)]
            logs = log_total[at, :]
            made = []
            for which, low in enumerate(range(0, LANES, HEAD_DIM)):
                part = slice(low, low + HEAD_DIM)
                scores = scaled_scores(q_pair[:, part], k_pair[:, part], same)
                top = jnp.max(scores, axis=1, keepdims=True)
                exponent = jnp.exp(scores - top)
                total = jnp.sum(exponent, axis=1, keepdims=True)
                probs = (exponent / total).astype(jnp.bfloat16)
                made.append(mul(probs, v_pair[:, part], ((1,), (0,))))
                head = i * (LANES // HEAD_DIM) + which
                logs = jnp.where(lane == head, top + jnp.log(total), logs)
            context[at, pair_at(first, 0)] = jnp.concatenate(made, axis=1).astype(jnp.bfloat16)
            log_total[at, :] = logs
        return carry

    lax.fori_loop(0, cols // LANES, pair, 0)


def attention_back_kernel(
    chunk, joined, context_low, log_total, seg_col, seg_row, joined_grad, column_sums
):
    length, cols = context_low.shape
    lane = lax.broadcasted_iota(jnp.int32, (chunk, LANES), 1)

    def pair(i, carry):
        first = i * LANES
        k_pair = joined[:, pair_at(first, cols)]
        v_pair = joined[:, pair_at(first, 2 * cols)]
        key_sums = [None] * (LANES // HEAD_DIM)
        value_sums = [None] * (LANES // HEAD_DIM)
        query_column = jnp.zeros((1, LANES), jnp.float32)
        for start in range(0, length, chunk):
            at = pl.ds(start, chunk)
            same = seg_col[at, :] == seg_row[...]
            q_pair = joined[at, pair_at(first, 0)]
            c_pair = context_low[at, pair_at(first, 0)]
            logs = log_total[at, :]
            made = []
            for which, low in enumerate(range(0, LANES, HEAD_DIM)):
                part = slice(low, low + HEAD_DIM)
                q, k, v, c = q_pair[:, part], k_pair[:, part], v_pair[:, part], c_pair[:, part]
                head = i * (LANES // HEAD_DIM) + which
                log_sum = jnp.sum(jnp.where(lane == head, logs, 0.0), axis=1, keepdims=True)
                probabilities = jnp.exp(scaled_scores(q, k, same) - log_sum)
                prob_grad = mul(c, v, ((1,), (1,)))
                row_delta = jnp.sum(prob_grad * probabilities, axis=1, keepdims=True)
                score_grad = (probabilities * (prob_grad - row_delta)).astype(jnp.bfloat16)
                value_part = mul(probabilities.astype(jnp.bfloat16), c, ((0,), (0,)))
                key_part = mul(score_grad, q, ((0,), (0,)))
                made.append(mul(score_grad, k, ((1,), (0,))))
                if start:
                    value_part = value_part + value_sums[which]
                    key_part = key_part + key_sums[which]
                value_sums[which] = value_part
                key_sums[which] = key_part
            query_grad = (jnp.concatenate(made, axis=1) * SCORE_SCALE).astype(jnp.bfloat16)
            joined_grad[at, pair_at(first, 0)] = query_grad
            query_column = query_column + jnp.sum(
                query_grad.astype(jnp.float32), axis=0, keepdims=True
            )
        key_grad = (jnp.concatenate(key_sums, axis=1) * SCORE_SCALE).astype(jnp.bfloat16)
        value_grad = jnp.concatenate(value_sums, axis=1).astype(jnp.bfloat16)
        joined_grad[:, pair_at(first, cols)] = key_grad
        joined_grad[:, pair_at(first, 2 * cols)] = value_grad
        column_sums[0:1, pair_at(first, 0)] = query_column
        column_sums[1:2, pair_at(first, 0)] = jnp.sum(
            value_grad.astype(jnp.float32), axis=0, keepdims=True
        )
        return carry

    lax.fori_loop(0, cols // LANES, pair, 0)


def local_kernel(body, shapes, work, name, *arrays):
    vmem = pl.BlockSpec(memory_space=pltpu.VMEM)
    return pl.pallas_call(
        body,
        out_shape=shapes,
        in_specs=[vmem] * len(arrays),
        out_specs=tuple(vmem for _ in shapes),
        compiler_params=pltpu.CompilerParams(vmem_limit_bytes=40 * 1024 * 1024),
        cost_estimate=pl.CostEstimate(flops=work, bytes_accessed=1 << 22, transcendentals=1 << 21),
        name=name,
    )(*arrays)


def pair_sum(rows, tp_rank):
    layers, depth, cols = rows.shape
    halves = rows.reshape(layers, 2, depth // 2, cols)
    away = lax.dynamic_index_in_dim(halves, 1 - tp_rank, 1, keepdims=False)
    mine = lax.dynamic_index_in_dim(halves, tp_rank, 1, keepdims=False)
    return mine + lax.ppermute(away, "tp", [(0, 1), (1, 0)])


def per_device(
    block_input,
    cotangent,
    qkv_weight,
    proj_weight,
    fc1_weight,
    fc2_weight,
    norm_gains,
    biases,
    fc1_bias,
    segments,
    keep_flags,
):
    local_len, row_count, width = block_input.shape
    assert row_count == 1
    tp_rank = lax.axis_index("tp")
    tp_size = lax.axis_size("tp")
    full_len = local_len * tp_size
    shard_rows = qkv_weight.shape[1]
    head_cols = qkv_weight.shape[3]
    ff_cols = fc1_weight.shape[2]
    qkv_end = 3 * head_cols
    proj_end = qkv_end + head_cols
    fc1_end = proj_end + ff_cols
    bf16 = jnp.bfloat16
    f32 = jnp.float32

    segment_row = segments[0]
    local_segments = lax.dynamic_slice_in_dim(segment_row, tp_rank * local_len, local_len, 0)
    member = (
        local_segments[:, None] == jnp.arange(SEGS, dtype=jnp.int32)[None, :]
    ).astype(f32)

    def token_keep(keep_row):
        return jnp.sum(member * keep_row.astype(f32), axis=1, keepdims=True)

    def place(part_grad, total_len):
        return lax.dynamic_update_slice_in_dim(
            jnp.zeros((total_len,), f32), part_grad, tp_rank * part_grad.shape[0], 0
        )

    def gather_positions(local_rows):
        return lax.all_gather(local_rows, "tp", axis=0, tiled=True)

    def scatter_positions(partial):
        if tp_size == 2:
            halves = partial.reshape(2, local_len, width)
            away = lax.dynamic_index_in_dim(halves, 1 - tp_rank, 0, keepdims=False)
            mine = lax.dynamic_index_in_dim(halves, tp_rank, 0, keepdims=False)
            arrived = lax.ppermute(away, "tp", [(0, 1), (1, 0)])
            return mine.astype(f32) + arrived.astype(f32)
        return lax.psum_scatter(partial, "tp", scatter_dimension=0, tiled=True).astype(f32)

    row_devices = lax.axis_size("rows")
    own_kernels = shard_rows % 16 == 0 and row_devices % 4 == 0 and tp_size == 2
    shards = (
        [
            jnp.concatenate(
                [
                    qkv_weight[layer].reshape(shard_rows, qkv_end).astype(bf16),
                    proj_weight[layer].T.astype(bf16),
                    fc1_weight[layer].astype(bf16),
                    fc2_weight[layer].T.astype(bf16),
                ],
                axis=1,
            )
            for layer in range(LAYERS)
        ]
    )
    vector_parts = [norm_gains, biases, fc1_bias[:, None, :]]
    vector_flat = jnp.concatenate([part.reshape(-1) for part in vector_parts])
    if own_kernels:
        filled = -(-vector_flat.size // (8 * LANES)) * 8 * LANES
        packed_first, vector_full = gather_rows(
            shards[0][None],
            jnp.pad(vector_flat, (0, filled - vector_flat.size)).reshape(-1, LANES),
            row_devices // 4,
        )
        vector_full = vector_full.reshape(row_devices * tp_size, -1)
        packed_full = [packed_first[0]] + [
            lax.all_gather(shard, "rows", axis=0, tiled=True) for shard in shards[1:]
        ]
    else:
        packed_full = [lax.all_gather(shard, "rows", axis=0, tiled=True) for shard in shards]
        vector_full = lax.all_gather(vector_flat, ("rows", "tp"), axis=0, tiled=False)
    full_vectors = []
    first = 0
    for part in vector_parts:
        taken = vector_full[:, first : first + part.size].reshape((-1,) + part.shape)
        first += part.size
        full_vectors.append(jnp.moveaxis(taken, 0, 2).reshape(part.shape[0], part.shape[1], -1))
    gains_full, biases_full, fc1_bias_full = full_vectors

    stream = block_input[:, 0]
    saved = []
    for layer in range(LAYERS):
        packed = packed_full[layer]
        w_qkv = packed[:, :qkv_end]
        w_proj = packed[:, qkv_end:proj_end]
        w_fc1 = packed[:, proj_end:fc1_end]
        w_fc2 = packed[:, fc1_end:]
        gain = gains_full[layer]
        bias = biases_full[layer]
        in_bias = jnp.concatenate(
            [
                lax.dynamic_slice_in_dim(bias[1], tp_rank * head_cols, head_cols, 0),
                jnp.zeros((head_cols,), f32),
                lax.dynamic_slice_in_dim(bias[2], tp_rank * head_cols, head_cols, 0),
            ]
        )
        up_bias = lax.dynamic_slice_in_dim(fc1_bias_full[layer, 0], tp_rank * ff_cols, ff_cols, 0)
        keep_attn = token_keep(keep_flags[layer, 0])
        keep_mlp = token_keep(keep_flags[layer, 1])
        xhat_one, rstd_one = apply_layer_norm(stream)
        normed_one = gather_positions((xhat_one * gain[0] + bias[0]).astype(bf16))
        joined = (mul(normed_one, w_qkv, ((1,), (0,))) + in_bias).astype(bf16)
        context, log_total = local_kernel(
            functools.partial(attention_kernel, full_len // 2),
            (
                jax.ShapeDtypeStruct((full_len, head_cols), bf16),
                jax.ShapeDtypeStruct((full_len, LANES), f32),
            ),
            4 * full_len * full_len * head_cols,
            "attention",
            joined,
            segment_row[:, None],
            segment_row[None],
        )
        attn = scatter_positions(mul(context, w_proj, ((1,), (1,))).astype(bf16)) + bias[3]
        middle = stream + keep_attn * attn / KEEP_RATE
        xhat_two, rstd_two = apply_layer_norm(middle)
        normed_two = gather_positions((xhat_two * gain[1] + bias[4]).astype(bf16))
        hidden_pre = mul(normed_two, w_fc1, ((1,), (0,))) + up_bias
        hidden = (hidden_pre * cumulative(hidden_pre)).astype(bf16)
        mlp = scatter_positions(mul(hidden, w_fc2, ((1,), (1,))).astype(bf16)) + bias[5]
        stream = middle + keep_mlp * mlp / KEEP_RATE
        saved.append(
            (
                (w_qkv, w_proj, w_fc1, w_fc2, gain, keep_attn, keep_mlp),
                (xhat_one, rstd_one, normed_one, joined, log_total, context),
                (xhat_two, rstd_two, normed_two, hidden_pre, hidden),
            )
        )

    grad = cotangent[:, 0]
    early_sums = [None] * LAYERS
    late_pairs = []
    all_vectors = []
    for layer in reversed(range(LAYERS)):
        (w_qkv, w_proj, w_fc1, w_fc2, gain, keep_attn, keep_mlp), attn_side, mlp_side = saved[layer]
        xhat_one, rstd_one, normed_one, joined, log_total, context = attn_side
        xhat_two, rstd_two, normed_two, hidden_pre, hidden = mlp_side
        mlp_grad = grad * keep_mlp / KEEP_RATE
        fc2_bias_grad = jnp.sum(mlp_grad, axis=0)
        mlp_low = gather_positions(mlp_grad.astype(bf16))
        hidden_grad = mul(mlp_low, w_fc2, ((1,), (0,)))
        pre_grad = (hidden_grad * gelu_slope(hidden_pre)).astype(bf16)
        if layer:
            packed = pack_products([(normed_two, pre_grad), (mlp_low, hidden)])
            packed, pre_grad = lax.optimization_barrier((packed, pre_grad))
            early_sums[layer] = lax.psum_scatter(
                packed, "rows", scatter_dimension=0, tiled=True
            ).astype(f32)
        fc1_bias_grad = jnp.sum(pre_grad.astype(f32), axis=0)
        two_grad = scatter_positions(mul(pre_grad, w_fc1, ((1,), (1,))).astype(bf16))
        gain_two_grad = jnp.sum(two_grad * xhat_two, axis=0)
        shift_two_grad = jnp.sum(two_grad, axis=0)
        middle_grad = grad + norm_backward(two_grad, xhat_two, rstd_two, gain[1])
        attn_grad = middle_grad * keep_attn / KEEP_RATE
        proj_bias_grad = jnp.sum(attn_grad, axis=0)
        attn_low = gather_positions(attn_grad.astype(bf16))
        context_low = mul(attn_low, w_proj, ((1,), (0,))).astype(bf16)
        joined_grad, in_bias_grad = local_kernel(
            functools.partial(attention_back_kernel, full_len // 2),
            (
                jax.ShapeDtypeStruct((full_len, 3 * head_cols), bf16),
                jax.ShapeDtypeStruct((2, head_cols), f32),
            ),
            10 * full_len * full_len * head_cols,
            "attention_back",
            joined,
            context_low,
            log_total,
            segment_row[:, None],
            segment_row[None],
        )
        one_grad = scatter_positions(mul(joined_grad, w_qkv, ((1,), (1,))).astype(bf16))
        gain_one_grad = jnp.sum(one_grad * xhat_one, axis=0)
        shift_one_grad = jnp.sum(one_grad, axis=0)
        grad = middle_grad + norm_backward(one_grad, xhat_one, rstd_one, gain[0])
        all_vectors += [
            gain_one_grad[None],
            gain_two_grad[None],
            shift_one_grad[None],
            place(in_bias_grad[0], width)[None],
            place(in_bias_grad[1], width)[None],
            proj_bias_grad[None],
            shift_two_grad[None],
            fc2_bias_grad[None],
            place(fc1_bias_grad, ff_cols * tp_size).reshape(width, -1).T,
        ]
        late_pairs += [(normed_one, joined_grad), (attn_low, context)]
        if not layer:
            late_pairs += [(normed_two, pre_grad), (mlp_low, hidden)]

    vector_count = 8 + ff_cols * tp_size // width
    vector_rows = jnp.concatenate(all_vectors, axis=0)
    vector_rows = jnp.pad(vector_rows, ((0, LANES - vector_rows.shape[0]), (0, 0)))
    if own_kernels:
        qkv_out, proj_out, fc1_late, fc2_late, late_vectors = sum_rows(
            late_pairs, vector_rows, row_devices // 4
        )
        qkv_out = jnp.transpose(qkv_out, (0, 2, 1, 3))
        proj_out = jnp.transpose(proj_out, (0, 2, 1))
        fc2_late = fc2_late.T
    else:
        late_sum = lax.psum_scatter(
            pack_products(late_pairs, vector_rows), "rows", scatter_dimension=0, tiled=True
        ).astype(f32)
        both_layers = [
            late_sum[:, layer * proj_end : (layer + 1) * proj_end]
            for layer in reversed(range(LAYERS))
        ]
        qkv_out = jnp.stack(
            [part[:, :qkv_end].reshape(shard_rows, 3, head_cols) for part in both_layers]
        )
        proj_out = jnp.stack([part[:, qkv_end:].T for part in both_layers])
        rest = late_sum[:, LAYERS * proj_end :]
        fc1_late = rest[:, :ff_cols]
        fc2_late = rest[:, ff_cols : 2 * ff_cols].T
        late_vectors = rest[:, 2 * ff_cols :]
    fc1_out = jnp.stack([fc1_late] + [part[:, :ff_cols] for part in early_sums[1:]])
    fc2_out = jnp.stack([fc2_late] + [part[:, ff_cols:].T for part in early_sums[1:]])
    late_vectors = late_vectors[None]
    if tp_size == 2:
        late_vectors = pair_sum(late_vectors, tp_rank)[0]
    else:
        late_vectors = lax.psum_scatter(
            late_vectors, "tp", scatter_dimension=1, tiled=True
        )[0]
    vector_sums = [
        late_vectors[:, layer * vector_count : (layer + 1) * vector_count]
        for layer in reversed(range(LAYERS))
    ]
    return (
        stream[:, None],
        grad[:, None],
        qkv_out,
        proj_out,
        fc1_out,
        fc2_out,
        jnp.stack([part[:, :2].T for part in vector_sums]),
        jnp.stack([part[:, 2:8].T for part in vector_sums]),
        jnp.stack([part[:, 8:].reshape(-1) for part in vector_sums]),
    )


def solution(mesh):
    placed = (
        P("tp", "rows", None),
        P("tp", "rows", None),
        P(None, "rows", None, "tp"),
        P(None, "tp", "rows"),
        P(None, "rows", "tp"),
        P(None, "tp", "rows"),
        P(None, None, ("rows", "tp")),
        P(None, None, ("rows", "tp")),
        P(None, ("rows", "tp")),
        P("rows", None),
        P(None, None, "rows", None),
    )
    return jax.shard_map(
        per_device,
        mesh=mesh,
        in_specs=placed,
        out_specs=placed[:2] + placed[2:9],
        check_vma=False,
    )
```
